128 devices in a mesh: rep: 1, r: 16 (over y, z), s: 8 (over x, core).
Axes of the slice: x: 4, y: 4, z: 4, core: 2. Of those that a mesh axis runs over, the one named last changes fastest.
Arguments:
- x: bfloat16 [128, 2048, 1024], P(('rep', 'r', 's'))
- dy: bfloat16 [128, 2048, 1024], P(('rep', 'r', 's'))
- w_gate: bfloat16 [2, 1024, 3200], P(None, 's')
- w_up: bfloat16 [2, 1024, 3200], P(None, 's')
- w_down: bfloat16 [2, 3200, 1024], P(None, 's')
- m_w_gate: float32 [2, 1024, 3200], P(None, 's')
- m_w_up: float32 [2, 1024, 3200], P(None, 's')
- m_w_down: float32 [2, 3200, 1024], P(None, 's')
- v_w_gate: float32 [2, 1024, 3200], P(None, 's')
- v_w_up: float32 [2, 1024, 3200], P(None, 's')
- v_w_down: float32 [2, 3200, 1024], P(None, 's')
Outputs:
- output 1: bfloat16 [2, 1024, 3200], P('rep', 's')
- output 2: bfloat16 [2, 1024, 3200], P('rep', 's')
- output 3: bfloat16 [2, 3200, 1024], P('rep', 's')
- output 4: float32 [2, 1024, 3200], P('rep', 's')
- output 5: float32 [2, 1024, 3200], P('rep', 's')
- output 6: float32 [2, 3200, 1024], P('rep', 's')
- output 7: float32 [2, 1024, 3200], P('rep', 's')
- output 8: float32 [2, 1024, 3200], P('rep', 's')
- output 9: float32 [2, 3200, 1024], P('rep', 's')
All inputs are finite; a program needn't handle non-finite values.
Results may differ from the reference program's by a relative error of at most 0.022.
Values are sent between devices in bfloat16 or wider.
A program may use at most 1.5 GiB of HBM per device.

```python
import jax
import jax.numpy as jnp
from jax import lax

SEQUENCES = 128
TOKENS = 2048
D = 1024
FF = 3200
LAYERS = 2
NAMES = ("w_gate", "w_up", "w_down")
SHAPES = {"w_gate": (LAYERS, D, FF), "w_up": (LAYERS, D, FF), "w_down": (LAYERS, FF, D)}


def bump(key, n, height):
    away = (jnp.arange(n, dtype=jnp.int32) - jax.random.randint(key, (), 0, n, jnp.int32)) % n
    return jnp.where(away < n // 8, height, 1.0)


def together(key, own, strength):
    shared = jax.random.normal(key, own.shape[1:], jnp.float32)
    return (own + strength * shared) * lax.rsqrt(1 + strength * strength)


def setup_inputs(seed: int = 0, part: int = 0) -> dict:
    kx, kdy, ka, kb, kz, kf, kh, kl, *keys = jax.random.split(jax.random.key(seed), 8 + 3 * len(NAMES))
    kx, kdy, ka, kb = (jax.random.fold_in(k, part) for k in (kx, kdy, ka, kb))
    kw, km, kv = (keys[i::3] for i in range(3))
    shape = (SEQUENCES, TOKENS, D)
    much_x, much_dy = jax.random.uniform(kz, (2,), jnp.float32, 0.0, 1.0)
    loud = 2.0 ** jax.random.uniform(jax.random.fold_in(kz, 1), (), jnp.float32, -1.0, 2.0)
    layers = 2.0 ** jax.random.uniform(kl, (LAYERS, 1, 1), jnp.float32, -1.0, 1.0)
    x = together(ka, jax.random.normal(kx, shape, jnp.float32), much_x) * bump(kf, D, 4.0)
    dy = together(kb, jax.random.normal(kdy, shape, jnp.float32), much_dy)
    drawn = {"x": x.astype(jnp.bfloat16), "dy": (loud * dy * (SEQUENCES * TOKENS) ** -0.5).astype(jnp.bfloat16)}
    for key, name in zip(kw, NAMES, strict=True):
        w = jax.random.normal(key, SHAPES[name], jnp.float32) * SHAPES[name][1] ** -0.5
        drawn[name] = (w * {"w_gate": 1.0, "w_up": bump(kh, FF, 4.0), "w_down": layers}[name]).astype(jnp.bfloat16)
    for key, name in zip(km, NAMES, strict=True):
        drawn[f"m_{name}"] = 0.1 * jax.random.normal(key, SHAPES[name], jnp.float32)
    for key, name in zip(kv, NAMES, strict=True):
        drawn[f"v_{name}"] = jax.random.uniform(key, SHAPES[name], jnp.float32, 0.005, 0.015)
    return drawn


def matmul(a, w):
    return jnp.dot(a, w, preferred_element_type=jnp.float32).astype(jnp.bfloat16)


def normed(h):
    wide = h.astype(jnp.float32)
    scale = lax.rsqrt(jnp.mean(wide**2, -1, keepdims=True) + 1e-6)
    return (wide * scale).astype(jnp.bfloat16)


def layer(h, w):
    a = normed(h)
    gate = jnp.dot(a, w["w_gate"], preferred_element_type=jnp.float32)
    up = jnp.dot(a, w["w_up"], preferred_element_type=jnp.float32)
    return h + matmul((jax.nn.silu(gate) * up).astype(jnp.bfloat16), w["w_down"])


def adamw(w, m, v, g):
    m = 0.9 * m + 0.1 * g
    v = 0.95 * v + 0.05 * g * g
    step = m * lax.rsqrt(v + 1e-8) + 0.1 * w
    return (w - 0.02 * step).astype(jnp.bfloat16), m, v


def clipped(gradients, sum_of_squares, count):
    factor = jnp.minimum(1.0, 0.5 * lax.rsqrt(sum_of_squares / count + 1e-30))
    return [g * factor for g in gradients]


def stack(weights, h):
    return lax.scan(lambda h, w: (layer(h, w), None), h, weights)[0]


def reference(x, dy, w_gate, w_up, w_down, m_w_gate, m_w_up, m_w_down, v_w_gate, v_w_up, v_w_down):
    weights = dict(zip(NAMES, (w_gate, w_up, w_down), strict=True))

    def take(so_far, sequence):
        h, by_y = sequence
        _, back = jax.vjp(lambda w: stack(w, h), weights)
        return jax.tree.map(lambda total, term: total + term.astype(jnp.float32), so_far, back(by_y)[0]), None

    none_yet = {name: jnp.zeros(w.shape, jnp.float32) for name, w in weights.items()}
    by_weights, _ = lax.scan(take, none_yet, (x, dy))
    gradients = [by_weights[name].astype(jnp.bfloat16).astype(jnp.float32) for name in NAMES]
    gradients = clipped(gradients, sum(jnp.sum(g * g) for g in gradients), sum(g.size for g in gradients))
    new = [
        adamw(w.astype(jnp.float32), m, v, g)
        for w, m, v, g in zip((w_gate, w_up, w_down), (m_w_gate, m_w_up, m_w_down), (v_w_gate, v_w_up, v_w_down), gradients, strict=True)
    ]
    return tuple(one[which] for which in range(3) for one in new)
```

```python
import sys
import jax
import jax.numpy as jnp
from jax import lax
from jax.sharding import PartitionSpec as P
import functools
import jax, jax.numpy as jnp
from jax import lax
from jax.experimental import pallas as pl
from jax.experimental.pallas import tpu as pltpu
bf=jnp.bfloat16; f32=jnp.float32
MESH=pl.DeviceIdType.MESH
T,D,F,TF=2048,1024,3200,640
NT=F//TF
NU=6*NT
LANES=128
def sds(s,d): return jax.ShapeDtypeStruct(s,d)
def dg_(a,b,ca,cb): return lax.dot_general(a,b,(((ca,),(cb,)),((),())),preferred_element_type=f32)
def coords():
    r=lax.axis_index("r"); s=lax.axis_index("s")
    return s//2, r//4, r%4, s%2
def dev(x,y,z,c): return (0,y*4+z,x*2+c)
def p2_body(dyp,ap,wg,wu,wd,hT,dgT,duT,tok):
    for h in range(T//tok):
        t=pl.ds(h*tok,tok)
        g=dg_(wg[...],ap[t,:],0,1); u=dg_(wu[...],ap[t,:],0,1)
        dh=dg_(wd[...],dyp[t,:],1,1).astype(bf).astype(f32)
        sg=jax.nn.sigmoid(g); si=g*sg
        hT[:,t]=(si*u).astype(bf)
        duT[:,t]=(dh*si).astype(bf)
        dgT[:,t]=(dh*u*(sg+si*(1-sg))).astype(bf)

def kb_kernel(dy_h,a1p_h,h1p_h,a0p_h,wg_h,wu_h,wd1_h,wd0_h,g_h,u_h,
              gt_o,gd_o,sq_o,
              dyp,ap,acc,wgb,wub,wdb,hT,dgT,duT,G,R0,Pb,R1,Q,R2,U,R3,GT,hb,sqa,
              lsem,wsem,gsem,osem,
              s0s,s0r,s1s,s1r,s2s,s2r,s3s,s3r,s4s,s4r,a2s,a2r):
    x,y,z,c=coords()
    me=x*2+c
    def ydev(d): return dev(x,(y+d)%4,z,c)
    def zdev(d): return dev(x,y,(z+d)%4,c)
    def xdev(d): return dev((x+d)%4,y,z,c)
    part=dev(x,y,z,1-c)
    bar=pltpu.get_barrier_semaphore()
    peers=[part]+[f(d) for f in (xdev,ydev,zdev) for d in (1,2,3)]+[dev((x+d)%4,y,z,1-c) for d in (1,2,3)]
    for p in peers: pl.semaphore_signal(bar,inc=1,device_id=p,device_id_type=MESH)
    def cpy(src,dst,sem): return pltpu.make_async_copy(src,dst,sem)
    def perm_cols(src,dst,sem,rows):
        return [cpy(src.at[rows,pl.ds((xx*2+cc)*LANES,LANES)],dst.at[:,pl.ds((cc*4+xx)*LANES,LANES)],sem) for xx in range(4) for cc in range(2)]
    def perm_rows(src,dst,sem,cols):
        return [cpy(src.at[pl.ds((xx*2+cc)*LANES,LANES),cols],dst.at[pl.ds((cc*4+xx)*LANES,LANES),:],sem) for xx in range(4) for cc in range(2)]
    allrows=pl.ds(0,T)
    dyl=perm_cols(dy_h,dyp,lsem.at[0],allrows)
    al=cpy(a1p_h,ap,lsem.at[1])
    def ft(j): return pl.ds(pl.multiple_of(j*TF,TF),TF)
    def wloads1(j,b):
        return (perm_rows(wg_h,wgb.at[b],wsem.at[0,b],ft(j))+perm_rows(wu_h,wub.at[b],wsem.at[1,b],ft(j))
               +perm_cols(wd1_h,wdb.at[b],wsem.at[2,b],ft(j)))
    def wwait1(b):
        cpy(wgb.at[b],wgb.at[b],wsem.at[0,b]).wait(); cpy(wub.at[b],wub.at[b],wsem.at[1,b]).wait(); cpy(wdb.at[b],wdb.at[b],wsem.at[2,b]).wait()
    def wloads0(j,b): return perm_cols(wd0_h,wdb.at[b],wsem.at[2,b],ft(j))
    for q in dyl: q.start()
    al.start()
    for q in wloads1(0,0): q.start()
    acc[...]=jnp.zeros_like(acc)
    sqa[...]=jnp.zeros_like(sqa)
    pl.semaphore_wait(bar,len(peers))

    RD=pltpu.make_async_remote_copy
    def rd(src,dst,ss,rs,d): return RD(src_ref=src,dst_ref=dst,send_sem=ss,recv_sem=rs,device_id=d,device_id_type=MESH)
    def c0(u):
        b=u%2
        return rd(G.at[b,:,pl.ds(pl.multiple_of((1-c)*512,512),512)],R0.at[b],s0s.at[b],s0r.at[b],part)
    def c1(u):
        b=u%2; o=[]
        for d in (1,2,3):
            o.append(rd(Pb.at[0,(y+d)%4],R1.at[b,0,d-1],s1s.at[0,d-1],s1r.at[b,0,d-1],ydev(d)))
            o.append(rd(Pb.at[1,(z+d)%4],R1.at[b,1,d-1],s1s.at[1,d-1],s1r.at[b,1,d-1],zdev(d)))
        return o
    def c2(u):
        b=u%2
        return [rd(Q.at[(x+d)%4],R2.at[b,d-1],s2s.at[d-1],s2r.at[b,d-1],xdev(d)) for d in (1,2,3)]
    def c3(u):
        b=u%2; o=[]
        for d in (1,2,3):
            o.append((rd(U.at[0],R3.at[b,0,z],s3s.at[0,d-1],s3r.at[b,0,z],zdev(d)),rd(U.at[0],R3.at[b,0,(z+d)%4],s3s.at[0,d-1],s3r.at[b,0,(z+d)%4],zdev(d))))
            o.append((rd(U.at[1],R3.at[b,1,y],s3s.at[1,d-1],s3r.at[b,1,y],ydev(d)),rd(U.at[1],R3.at[b,1,(y+d)%4],s3s.at[1,d-1],s3r.at[b,1,(y+d)%4],ydev(d))))
        return o
    def rowsA(q): return pl.ds(pl.multiple_of(q*80,80),80)
    def rowsB(q): return pl.ds(pl.multiple_of(320+q*80,80),80)
    def c4(u):
        b=u%2; o=[]
        for d in (1,2,3):
            o.append(rd(GT.at[u,rowsA(y)],GT.at[u,rowsA(y)],s4s.at[0,d-1],s4r.at[b,0,d-1],ydev(d)))
            o.append(rd(GT.at[u,rowsB(z)],GT.at[u,rowsB(z)],s4s.at[1,d-1],s4r.at[b,1,d-1],zdev(d)))
        return o
    def S0(u): c0(u).start()
    def S1(u):
        b=u%2
        c0(u).wait()
        for h in range(2):
            for q in range(4):
                for xx in range(4):
                    r=pl.ds(h*320+q*80,80)
                    own=G[b,r,pl.ds(pl.multiple_of(c*512+xx*128,128),128)]
                    Pb[h,q,xx]=(own.astype(f32)+R0[b,r,pl.ds(xx*128,128)].astype(f32)).astype(bf)
        for q in c1(u): q.start()
    def S2(u):
        b=u%2
        for q in c1(u): q.wait()
        for h,me_q in ((0,y),(1,z)):
            for xx in range(4):
                s=Pb[h,me_q,xx].astype(f32)
                for d in range(3): s=s+R1[b,h,d,xx].astype(f32)
                Q[xx,h]=s.astype(bf)
        for q in c2(u): q.start()
    def S3(u):
        b=u%2
        for q in c2(u): q.wait()
        for h in range(2):
            s=Q[x,h].astype(f32)
            for d in range(3): s=s+R2[b,d,h].astype(f32)
            s=s.astype(bf)
            U[h]=s
        for q,_ in c3(u): q.start()
    def S4(u):
        b=u%2
        for sd,rv in c3(u):
            sd.wait_send(); rv.wait_recv()
        R3[b,0,z]=U[0]
        R3[b,1,y]=U[1]
        for h,rows in ((0,rowsA(y)),(1,rowsB(z))):
            s=R3[b,h,0].astype(f32)
            for d in range(1,4): s=s+R3[b,h,d].astype(f32)
            GT[u,rows]=s.astype(bf)
        for q in c4(u): q.start()
    def blk(u,i):
        lay=u//15; j=(u%15)//3
        n=8*j+i; own=n//5; row=(n%5)*80
        return lay,own,row
    def a2a(u,i):
        lay,own,row=blk(u,i)
        src=GT.at[u,pl.ds(i*80,80)]
        dst=gd_o.at[1-lay,pl.ds(pl.multiple_of(row,80),80),pl.ds(pl.multiple_of(me*128,128),128)]
        return rd(src,dst,a2s,a2r.at[lay],(0,y*4+z,own)),cpy(src,dst,osem.at[1])
    def S5(u):
        for q in c4(u): q.wait()
        v=GT[u].astype(f32)
        sqa[...]+=jnp.sum((v*v).reshape(80,8,128),axis=0)
        down=(u%3)==0
        @pl.when(jnp.logical_not(down))
        def _(): cpy(GT.at[u],gt_o.at[u],osem.at[0]).start()
        @pl.when(down)
        def _():
            for i in range(8):
                lay,own,row=blk(u,i)
                r_,l_=a2a(u,i)
                @pl.when(own!=me)
                def _(): r_.start()
                @pl.when(own==me)
                def _(): l_.start()
    def slot(t,last=False):
        for k,S in ((5,S5),(4,S4),(3,S3),(2,S2),(1,S1)):
            u=t-k
            @pl.when(jnp.logical_and(u>=0,u<NU))
            def _(): S(u)
        if not last: S0(t)

    for q in dyl[:1]:
        cpy(dyp,dyp,lsem.at[0]).wait()
    al.wait()
    tok=1024
    def step2(j,_):
        b=j%2
        wwait1(b)
        @pl.when(j+1<NT)
        def _():
            for q in wloads1(j+1,1-b): q.start()
        @pl.when(j+1==NT)
        def _():
            for q in wloads0(0,1-b): q.start()
        p2_body(dyp,ap,wgb.at[b],wub.at[b],wdb.at[b],hT,dgT,duT,tok)
        t=3*j
        G[t%2]=jnp.dot(hT[...],dyp[...],preferred_element_type=f32).astype(bf)
        slot(t)
        acc[...]+=dg_(dgT[...],wgb[b],0,1)
        G[(t+1)%2]=jnp.dot(dgT[...],ap[...],preferred_element_type=f32).astype(bf)
        slot(t+1)
        acc[...]+=dg_(duT[...],wub[b],0,1)
        G[(t+2)%2]=jnp.dot(duT[...],ap[...],preferred_element_type=f32).astype(bf)
        slot(t+2)
        return 0
    lax.fori_loop(0,NT,step2,0)
    a0l=cpy(a0p_h,ap,lsem.at[1]); a0l.start()
    CH=256
    def hl(i,b): return cpy(h1p_h.at[pl.ds(pl.multiple_of(i*CH,CH),CH)],hb.at[b],lsem.at[2+b])
    hl(0,0).start()
    def nb(i,_):
        b=i%2
        @pl.when(i+1<T//CH)
        def _(): hl(i+1,1-b).start()
        hl(i,b).wait()
        r=pl.ds(pl.multiple_of(i*CH,CH),CH)
        wide=hb[b].astype(f32)
        scale=lax.rsqrt(jnp.mean(wide*wide,-1,keepdims=True)+1e-6)
        da=acc[r,:].astype(bf).astype(f32)
        inner=jnp.mean(da*wide,-1,keepdims=True)
        dw=(da*scale-wide*(scale*scale*scale*inner)).astype(bf)
        dyp[r,:]=(dyp[r,:].astype(f32)+dw.astype(f32)).astype(bf)
        return 0
    lax.fori_loop(0,T//CH,nb,0)
    TK=512; NS=T//TK
    def guv(b,m): return acc.at[pl.ds(pl.multiple_of(b*TF,TF),TF),pl.ds(m*TK,TK)]
    def gul(i,b):
        j=i//NS; s=i%NS
        return [cpy(hh.at[ft(j),pl.ds(pl.multiple_of(s*TK,TK),TK)],guv(b,m),gsem.at[m,b]) for m,hh in ((0,g_h),(1,u_h))]
    for q in gul(0,0): q.start()
    a0l.wait()
    def step3(j,_):
        b=(NT+j)%2
        cpy(wdb.at[b],wdb.at[b],wsem.at[2,b]).wait()
        @pl.when(j+1<NT)
        def _():
            for q in wloads0(j+1,1-b): q.start()
        def sub(s,_):
            i=j*NS+s; gb=i%2
            @pl.when(i+1<NT*NS)
            def _():
                for q in gul(i+1,1-gb): q.start()
            for q in gul(i,gb): q.wait()
            t=pl.ds(pl.multiple_of(s*TK,TK),TK)
            dh=dg_(wdb[b],dyp[t,:],1,1).astype(bf).astype(f32)
            r=pl.ds(pl.multiple_of(gb*TF,TF),TF)
            g=acc[r,pl.ds(0,TK)]; u=acc[r,pl.ds(TK,TK)]
            sg=jax.nn.sigmoid(g); si=g*sg
            hT[:,t]=(si*u).astype(bf)
            duT[:,t]=(dh*si).astype(bf)
            dgT[:,t]=(dh*u*(sg+si*(1-sg))).astype(bf)
            return 0
        lax.fori_loop(0,NS,sub,0)
        t=15+3*j
        G[t%2]=jnp.dot(hT[...],dyp[...],preferred_element_type=f32).astype(bf)
        slot(t)
        G[(t+1)%2]=jnp.dot(dgT[...],ap[...],preferred_element_type=f32).astype(bf)
        slot(t+1)
        G[(t+2)%2]=jnp.dot(duT[...],ap[...],preferred_element_type=f32).astype(bf)
        slot(t+2)
        return 0
    lax.fori_loop(0,NT,step3,0)
    def dr(t,_):
        slot(t,True); return 0
    lax.fori_loop(NU,NU+5,dr,0)
    def drain(n,rows,sem): cpy(GT.at[pl.ds(0,n),pl.ds(0,rows)],GT.at[pl.ds(0,n),pl.ds(0,rows)],sem).wait()
    drain(20,TF,osem.at[0])
    drain(2,400,osem.at[1])
    drain(14,400,a2s)
    for lay in range(2): drain(7,400,a2r.at[lay])
    sq_o[...]=sqa[...]

def kb(dy,a1p,h1p,a0p,wg,wu,wd1,wd0,gT,uT,cid=3):
    any_=pl.BlockSpec(memory_space=pl.ANY)
    V=pltpu.VMEM; DMA=pltpu.SemaphoreType.DMA
    return pl.pallas_call(kb_kernel,
        out_shape=(sds((NU,TF,128),bf),sds((2,400,1024),bf),sds((8,128),f32)),
        in_specs=[any_]*10,out_specs=(any_,any_,pl.BlockSpec(memory_space=pltpu.VMEM)),
        scratch_shapes=[V((T,D),bf),V((T,D),bf),V((T,D),f32),V((2,D,TF),bf),V((2,D,TF),bf),V((2,TF,D),bf),
            V((TF,T),bf),V((TF,T),bf),V((TF,T),bf),V((2,TF,D),bf),V((2,TF,512),bf),
            V((2,4,4,80,128),bf),V((2,2,3,4,80,128),bf),V((4,2,80,128),bf),V((2,3,2,80,128),bf),V((2,80,128),bf),V((2,2,4,80,128),bf),
            V((NU,TF,128),bf),V((2,256,D),bf),V((8,128),f32),
            DMA((4,)),DMA((3,2)),DMA((2,2)),DMA((2,)),
            DMA((2,)),DMA((2,)),DMA((2,3)),DMA((2,2,3)),DMA((3,)),DMA((2,3)),DMA((2,3)),DMA((2,2,4)),DMA((2,3)),DMA((2,2,3)),DMA,DMA((2,))],
        compiler_params=pltpu.CompilerParams(collective_id=cid,has_side_effects=True,vmem_limit_bytes=67043328),
        cost_estimate=pl.CostEstimate(flops=12*2*T*D*F,bytes_accessed=150_000_000,transcendentals=0),
        name="backward")(dy,a1p,h1p,a0p,wg,wu,wd1,wd0,gT,uT)

NAMES = ("w_gate", "w_up", "w_down")

def cp(n=1,**k): return pltpu.CompilerParams(vmem_limit_bytes=63*1024*1024,dimension_semantics=("arbitrary",)*n,**k)
def p1(a,wg,wu,tok=1024):
    def k(a,wg,wu,gT,uT,hT):
        for h in range(T//tok):
            t=pl.ds(h*tok,tok)
            g=dg_(wg[...],a[t,:],0,1); u=dg_(wu[...],a[t,:],0,1)
            gT[:,t]=g; uT[:,t]=u
            hT[:,t]=(g*jax.nn.sigmoid(g)*u).astype(bf)
    o=pl.BlockSpec((TF,T),lambda j:(j,0))
    w=pl.BlockSpec((D,TF),lambda j:(0,j))
    return pl.pallas_call(k,grid=(NT,),in_specs=[pl.BlockSpec((T,D),lambda j:(0,0),pipeline_mode=pl.Buffered(1)),w,w],out_specs=(o,o,o),
        out_shape=(sds((F,T),f32),sds((F,T),f32),sds((F,T),bf)),compiler_params=cp(),name="gateup")(a,wg,wu)
def p1b(hT,wd,x,tm=512):
    def k(hT,wd,x,o):
        y=dg_(hT[...],wd[...],0,0).astype(bf)
        o[...]=x[...]+y
    return pl.pallas_call(k,grid=(T//tm,),in_specs=[pl.BlockSpec((F,tm),lambda i:(0,i)),pl.BlockSpec((F,D),lambda i:(0,0),pipeline_mode=pl.Buffered(1)),pl.BlockSpec((tm,D),lambda i:(i,0))],
       out_specs=pl.BlockSpec((tm,D),lambda i:(i,0)),out_shape=sds((T,D),bf),compiler_params=cp(),name="down")(hT,wd,x)

def normed(h):
    wide = h.astype(jnp.float32)
    scale = lax.rsqrt(jnp.mean(wide**2, -1, keepdims=True) + 1e-6)
    return (wide * scale).astype(jnp.bfloat16)
def adamw(w, m, v, g):
    m = 0.9 * m + 0.1 * g
    v = 0.95 * v + 0.05 * g * g
    step = m * lax.rsqrt(v + 1e-8) + 0.1 * w
    return (w - 0.02 * step).astype(jnp.bfloat16), m, v
def clipped(gradients, sum_of_squares, count):
    factor = jnp.minimum(1.0, 0.5 * lax.rsqrt(sum_of_squares / count + 1e-30))
    return [g * factor for g in gradients]

def solution(mesh):
    def fetched(weights, number):
        return [lax.all_gather(w[number], "s", axis=0, tiled=True) for w in weights]
    def perm(a): return a.reshape(T,4,2,128).transpose(0,2,1,3).reshape(T,D)
    def step(x, dy, *arrays):
        weights, m, v = (arrays[i : i + 3] for i in (0, 3, 6))
        x=x[0]; dy=dy[0]
        wg0,wu0,wd0=fetched(weights,0)
        wg1,wu1,wd1=fetched(weights,1)
        a0=normed(x)
        gT,uT,hT=p1(a0,wg0,wu0)
        h1=p1b(hT,wd0,x)
        a1=normed(h1)
        GT,GD,sq=kb(dy,perm(a1),perm(h1),perm(a0),wg1,wu1,wd1,wd0,gT,uT)
        GT=GT.reshape(2,5,3,640,128)
        def mat(i): return GT[::-1,:,i].reshape(2,3200,128).swapaxes(1,2)
        gradients=[mat(1).astype(f32),mat(2).astype(f32),GD.astype(f32)]
        squares = lax.psum(jnp.sum(sq), "s")
        gradients = clipped(gradients, squares, lax.psum(1, "s") * sum(g.size for g in gradients))
        new = [adamw(w.astype(jnp.float32), m, v, g) for w, m, v, g in zip(weights, m, v, gradients, strict=True)]
        return tuple(one[which] for which in range(3) for one in new)
    states, cut = P(("rep", "r", "s"), None, None), P(None, "s", None)
    return jax.shard_map(step,mesh=mesh,in_specs=(states, states) + (cut,) * 9,out_specs=(P("rep", "s", None),) * 9,check_vma=False)
```

```python
import jax, jax.numpy as jnp
from jax import lax
from jax.experimental import pallas as pl
from jax.experimental.pallas import tpu as pltpu
from jax.sharding import PartitionSpec as P

bf, f32 = jnp.bfloat16, jnp.float32
T, D, F, TF = 2048, 1024, 3200, 640
TWO, MATS, RING = 2, 3, 4
NT = F // TF
NU = TWO * MATS * NT
NA = TWO * NT + TWO
DEEP = 6
LANES, SUB, HALF, CH, SH = 128, 80, 512, 256, 400
DEV = D // LANES
TF2, TF3, TB, TK = TWO * TF, MATS * TF, T // TWO, T // RING
AROWS = LANES // DEV
OFFS = range(1, RING)
VMEM_LIMIT = 67043328
EPS = 1e-6
OFFLAY = NU // TWO


def sds(s, d): return jax.ShapeDtypeStruct(s, d)
def dot_(a, b, ca, cb): return lax.dot_general(a, b, (((ca,), (cb,)), ((), ())), preferred_element_type=f32)
def mul(i, n): return pl.multiple_of(i * n, n)
def blk(i, n): return pl.ds(mul(i, n), n)
def cut(n): return pl.ds(0, n)
def cpy(src, dst, sem): return pltpu.make_async_copy(src, dst, sem)
def wt(ref, sem): cpy(ref, ref, sem).wait()
def start(cs):
    for q in cs: q.start()
def each(lo, hi, f):
    def g(i, _):
        f(i)
        return _
    lax.fori_loop(lo, hi, g, 0)
def rms(wide): return lax.rsqrt(jnp.mean(wide * wide, -1, keepdims=True) + EPS)
def pc(k): return (k % TWO) * RING + k // TWO
def par(u): return u % TWO
def ring(u): return u % RING


def step_kernel(x_h, dy_h, wg_i, wu_i, wd_i,
                gt_o, gd_o, sq_o, WGU, WD, a0p_h, h1p_h, AB_h, h_h,
                ya, acc, wgu, wdb, H, G, R0, Pb, R1, Q, R2, U, R3, GT, sqa, SQ,
                dysem, asem, psem, ownsem, gusem, wdsem, stsem, hsem, gtsem, locsem,
                s0s, s0r, s1s, s1r, s2s, s2r, s3s, s3r, s4s, s4r, a2s, a2r,
                ag0s, ag0r, agds, agdr, ag1s, ag1r, ag2s, ag2r, sqs, sqr):
    r_, me = lax.axis_index("r"), lax.axis_index("s")
    x, y, z, c = me // TWO, r_ // RING, r_ % RING, me % TWO
    own = c * RING + x
    def dev(x, y, z, c): return (0, y * RING + z, x * TWO + c)
    def xdev(d): return dev(ring(x + d), y, z, c)
    def ydev(d): return dev(x, ring(y + d), z, c)
    def zdev(d): return dev(x, y, ring(z + d), c)
    part = dev(x, y, z, 1 - c)
    AX = ((0, y, ydev), (1, z, zdev))
    dyp, ap = ya.at[0], ya.at[1]
    bar = pltpu.get_barrier_semaphore()
    peers = [part] + [f(d) for f in (xdev, ydev, zdev) for d in OFFS] + [dev(ring(x + d), y, z, 1 - c) for d in OFFS]
    for p in peers: pl.semaphore_signal(bar, inc=1, device_id=p, device_id_type=pl.DeviceIdType.MESH)
    def rd(src, dst, ss, rs, d):
        return pltpu.make_async_remote_copy(src_ref=src, dst_ref=dst, send_sem=ss, recv_sem=rs, device_id=d, device_id_type=pl.DeviceIdType.MESH)
    def same(ref, ss, rs, d): return rd(ref, ref, ss, rs, d)
    def permuted(src, dst, sem): return [cpy(src.at[:, pl.ds(k * LANES, LANES)], dst.at[:, pl.ds(pc(k) * LANES, LANES)], sem) for k in range(DEV)]
    start(permuted(x_h, ap, psem))
    staged = [wdb.at[pl.ds(l * TF, SH)] for l in range(TWO)]
    for l in range(TWO): start(permuted(wd_i.at[l], staged[l], ownsem.at[l]))
    start(permuted(dy_h, dyp, dysem))
    sqa[...] = jnp.zeros_like(sqa)
    for l in range(TWO):
        wt(staged[l], ownsem.at[l])
        cpy(staged[l], WD.at[l, blk(me, SH), :], ownsem.at[l]).start()
    pl.semaphore_wait(bar, len(peers))

    def gu_load(l, j, b):
        for m, inp in enumerate((wg_i, wu_i)):
            cols = pl.ds(m * TF, TF)
            cpy(inp.at[l, :, blk(j, TF)], wgu.at[b, blk(own, LANES), cols], gusem.at[b]).start()
            def one(e):
                k = (own + e) % DEV
                cpy(WGU.at[l, k, m, :, blk(j, TF)], wgu.at[b, blk(k, LANES), cols], gusem.at[b]).start()
            each(1, DEV, one)
    def gu_wait(b): wt(wgu.at[b], gusem.at[b])
    def d_load(l, j, b): cpy(WD.at[l, blk(j, TF), :], wdb.at[blk(b, TF)], wdsem.at[b]).start()
    def d_wait(b): wt(wdb.at[blk(b, TF)], wdsem.at[b])

    def q16(h, q): return pl.ds(pl.multiple_of(h * (LANES // TWO) + q * AROWS, AROWS), AROWS)
    def colq(h, q): return blk(pc(RING * h + q), LANES)
    def fork(u, fg, fd):
        @pl.when(u % (NT + TWO) < NT)
        def _(): fg(u // (NT + TWO), u % (NT + TWO))
        @pl.when(u % (NT + TWO) >= NT)
        def _(): fd(u - NT)
    def wait6(ref, ss, rs, b):
        def one(i):
            h, d = i // MATS, i % MATS
            wt(ref, ss.at[b, h, d])
            wt(ref, rs.at[b, h, d])
        each(0, DEEP, one)
    def A0(u):
        b = u % DEEP
        def fg(l, j):
            for m, inp in enumerate((wg_i, wu_i)):
                def one(i):
                    for h, q, _ in AX: rd(inp.at[l, q16(h, q), blk(j, TF)], WGU.at[l, own, m, q16(h, q), blk(j, TF)], ag0s.at[b, h, i], ag0r.at[b, h, i], xdev(i + 1)).start()
                each(0, MATS, one)
                rd(inp.at[l, :, blk(j, TF)], WGU.at[l, own, m, :, blk(j, TF)], agds.at[u], agdr.at[u], part).start()
        def fd(l):
            wt(WD.at[0, cut(SH), :], ownsem.at[l])
            def one(i):
                for h, q, _ in AX: same(WD.at[l, blk(me, SH), colq(h, q)], ag0s.at[b, h, i], ag0r.at[b, h, i], xdev(i + 1)).start()
            each(0, MATS, one)
            same(WD.at[l, blk(me, SH), :], agds.at[u], agdr.at[u], part).start()
        fork(u, fg, fd)
    def A1(u):
        b = u % DEEP
        def fg(l, j):
            wait6(WGU.at[0, 0, :, cut(AROWS), cut(TF)], ag0s, ag0r, b)
            def one(i):
                k, d = c * RING + ring(x + i // MATS + 1), i % MATS
                for h, q, f in AX: same(WGU.at[l, k, :, q16(h, q), blk(j, TF)], ag1s.at[b, h, d], ag1r.at[b, h, d], f(d + 1)).start()
            each(0, MATS * MATS, one)
        def fd(l):
            wait6(WD.at[0, cut(SH), cut(LANES)], ag0s, ag0r, b)
            def one(i):
                k, d = TWO * ring(x + i // MATS + 1) + c, i % MATS
                for h, q, f in AX: same(WD.at[l, blk(k, SH), colq(h, q)], ag1s.at[b, h, d], ag1r.at[b, h, d], f(d + 1)).start()
            each(0, MATS * MATS, one)
        fork(u, fg, fd)
    gu1, gu3 = WGU.at[0, 0, :, :, cut(TF)], WGU.at[0, cut(MATS), :, :, cut(TF)]
    wd1, wd3 = WD.at[0, cut(SH), :], WD.at[0, cut(MATS * SH), :]
    def A2(u):
        b = u % DEEP
        def fg(l, j):
            wait6(WGU.at[0, cut(MATS), :, cut(AROWS), cut(TF)], ag1s, ag1r, b)
            each(1, RING, lambda i: same(WGU.at[l, c * RING + ring(x + i), :, :, blk(j, TF)], ag2s.at[b], ag2r.at[u], part).start())
        def fd(l):
            wait6(WD.at[0, cut(MATS * SH), cut(LANES)], ag1s, ag1r, b)
            each(1, RING, lambda i: same(WD.at[l, blk(TWO * ring(x + i) + c, SH), :], ag2s.at[b], ag2r.at[u], part).start())
        fork(u, fg, fd)
    def A3(u):
        b = u % DEEP
        def done(one, three):
            for ref, sem in ((one, agds.at[u]), (one, agdr.at[u]), (three, ag2s.at[b]), (three, ag2r.at[u])): wt(ref, sem)
        fork(u, lambda l, j: done(gu1, gu3), lambda l: done(wd1, wd3))
    def guard(A, u):
        @pl.when(jnp.logical_and(u >= 0, u < NA))
        def _(): A(u)

    def c0(u): return rd(G.at[par(u), :, blk(1 - c, HALF)], R0.at[ring(u)], s0s.at[par(u)], s0r.at[ring(u)], part)
    def c1(u):
        return [rd(Pb.at[par(u), h, ring(q + d)], R1.at[ring(u), h, d - 1], s1s.at[par(u), h, d - 1], s1r.at[ring(u), h, d - 1], f(d)) for d in OFFS for h, q, f in AX]
    def c2(u): return [rd(Q.at[par(u), ring(x + d)], R2.at[ring(u), d - 1], s2s.at[par(u), d - 1], s2r.at[ring(u), d - 1], xdev(d)) for d in OFFS]
    def c3(u, recv):
        o = []
        for d in OFFS:
            for h, q, f in ((0, z, zdev), (1, y, ydev)):
                k = ring(q + d) if recv else q
                o.append(rd(U.at[par(u), h], R3.at[ring(u), h, k], s3s.at[par(u), h, d - 1], s3r.at[ring(u), h, k], f(d)))
        return o
    def rows(h, q): return pl.ds(pl.multiple_of(h * (TF // TWO) + q * SUB, SUB), SUB)
    def c4(u):
        return [same(GT.at[u, rows(h, q)], s4s.at[par(u), h, d - 1], s4r.at[ring(u), h, d - 1], f(d)) for d in OFFS for h, q, f in AX]
    def S0(u): c0(u).start()
    def S1(u):
        c0(u).wait()
        def one(i):
            for k in range(RING):
                mine = G[par(u), blk(i, SUB), blk(c * RING + k, LANES)]
                Pb[par(u), i // RING, ring(i), k] = (mine.astype(f32) + R0[ring(u), blk(i, SUB), pl.ds(k * LANES, LANES)].astype(f32)).astype(bf)
        each(0, DEV, one)
        start(c1(u))
    def S2(u):
        for q in c1(u): q.wait()
        for h, mine, _ in AX:
            for k in range(RING):
                s = Pb[par(u), h, mine, k].astype(f32)
                for d in range(MATS): s = s + R1[ring(u), h, d, k].astype(f32)
                Q[par(u), k, h] = s.astype(bf)
        start(c2(u))
    def S3(u):
        for q in c2(u): q.wait()
        for h in range(TWO):
            s = Q[par(u), x, h].astype(f32)
            for d in range(MATS): s = s + R2[ring(u), d, h].astype(f32)
            U[par(u), h] = s.astype(bf)
        start(c3(u, False))
    def S4(u):
        for q in c3(u, False): q.wait_send()
        for q in c3(u, True): q.wait_recv()
        R3[ring(u), 0, z] = U[par(u), 0]
        R3[ring(u), 1, y] = U[par(u), 1]
        for h, q, _ in AX:
            s = R3[ring(u), h, 0].astype(f32)
            for d in OFFS: s = s + R3[ring(u), h, d].astype(f32)
            GT[u, rows(h, q)] = s.astype(bf)
        start(c4(u))
    def a2a(u, i):
        lay, n = u // OFFLAY, DEV * ((u % OFFLAY) // MATS) + i
        src, dst = GT.at[u, blk(i, SUB)], gd_o.at[1 - lay, blk(n % NT, SUB), blk(me, LANES)]
        return n // NT, rd(src, dst, a2s, a2r.at[lay], (0, r_, n // NT)), cpy(src, dst, locsem)
    def S5(u):
        for q in c4(u): q.wait()
        v = GT[u].astype(f32)
        sqa[...] += jnp.sum((v * v).reshape(SUB, DEV, LANES), axis=0)
        @pl.when(u % MATS > 0)
        def _(): cpy(GT.at[u], gt_o.at[u], gtsem).start()
        @pl.when(u % MATS == 0)
        def _():
            def one(i):
                @pl.when(a2a(u, i)[0] != me)
                def _(): a2a(u, i)[1].start()
                @pl.when(a2a(u, i)[0] == me)
                def _(): a2a(u, i)[TWO].start()
            each(0, DEV, one)
    STAGES = (S5, S4, S3, S2, S1)
    def slot(t):
        for i, S in enumerate(STAGES):
            u = t - TWO * (len(STAGES) - i)
            @pl.when(jnp.logical_and(u >= 0, u < NU))
            def _(): S(u)

    each(0, MATS, A0)
    wt(ap, psem)
    def xnorm(i):
        wide = ya[1, blk(i, CH), :].astype(f32)
        ya[1, blk(i, CH), :] = (wide * rms(wide)).astype(bf)
    each(0, T // CH, xnorm)
    cpy(ap, a0p_h, asem).start()
    def head(i):
        guard(A2, i - 1)
        @pl.when(i == 0)
        def _(): A1(i)
        A1(i + 1)
        A0(i + MATS)
    each(0, TWO, head)
    each(0, 1, A3)
    gu_load(0, 0, 0)
    each(MATS, RING, A1)
    each(NT, DEEP, A0)
    def stv(i): return acc.at[blk(i, TF), :]
    def step1(j):
        b = par(j)
        gu_wait(b)
        hs = j % MATS
        hr = blk(hs, TF)
        @pl.when(j >= MATS)
        def _(): wt(H.at[cut(TF)], hsem.at[hs])
        def sub(s):
            i = j * RING + s
            k = i % MATS
            @pl.when(i >= MATS)
            def _(): wt(stv(0), stsem.at[k])
            gu = dot_(wgu[b], ya[1, blk(s, TK), :], 0, 1)
            g, u = gu[:TF], gu[TF:]
            sg = jax.nn.sigmoid(g)
            si = g * sg
            acc[blk(k, TF), 0:TK] = si
            acc[blk(k, TF), TK:] = u * (sg + si * (1 - sg))
            H[hr, blk(s, TK)] = (si * u).astype(bf)
            cpy(stv(k), AB_h.at[i], stsem.at[k]).start()
            @pl.when(s == 0)
            def _(): guard(A2, j + 1)
            @pl.when(s == TWO)
            def _():
                guard(A3, j + 1)
                @pl.when(j < NT - 1)
                def _(): gu_load(0, j + 1, 1 - b)
                @pl.when(j == NT - 1)
                def _(): cpy(WD.at[0, pl.ds(TF3, TF2), :], wdb, wdsem.at[TWO]).start()
                guard(A1, j + RING)
                guard(A0, j + DEEP)
        each(0, RING, sub)
        cpy(H.at[hr], h_h.at[blk(j, TF), :], hsem.at[hs]).start()
    each(0, NT, step1)
    for i in range(MATS): wt(stv(0), stsem.at[i])
    wt(ap, asem)
    start(permuted(x_h, ap, psem))
    lo, mid = cut(TF2), wgu.at[0, cut(TF), cut(D)]
    cpy(WD.at[0, pl.ds(TF2, TF), :], mid, wdsem.at[0]).start()
    acc[...] = jnp.zeros_like(acc)
    def down(i):
        @pl.when(i == 1)
        def _(): wt(H.at[lo], hsem.at[MATS])
        wt(wdb, wdsem.at[TWO])
        def halves(h): acc[blk(h, TB), :] += dot_(H[lo, blk(h, TB)], wdb[...], 0, 0)
        each(0, TWO, halves)
        @pl.when(i == 0)
        def _():
            for k in range(TWO): wt(H.at[cut(TF)], hsem.at[k])
            cpy(h_h.at[lo], H.at[lo], hsem.at[MATS]).start()
            cpy(WD.at[0, lo, :], wdb, wdsem.at[TWO]).start()
            A2(i + DEEP)
            A1(i + NA - MATS)
            A0(i + NA - 1)
            wt(mid, wdsem.at[0])
            def halves(h): acc[blk(h, TB), :] += dot_(H[TF2:TF3, blk(h, TB)], wgu[0, 0:TF, 0:D], 0, 0)
            each(0, TWO, halves)
        A3(i + DEEP)
        A2(i + DEEP + 1)
        @pl.when(i == 0)
        def _(): A1(i + NA - TWO)
    each(0, TWO, down)
    gu_load(1, 0, 1)
    d_load(1, 0, 0)
    wt(H.at[cut(TF)], hsem.at[TWO])
    wt(ap, psem)
    def h1s(b): return G.at[b, cut(CH)]
    def fin(i):
        b, r = par(i), blk(i, CH)
        @pl.when(i >= TWO)
        def _(): wt(h1s(0), hsem.at[b])
        h1 = (ya[1, r, :].astype(f32) + acc[r, :].astype(bf).astype(f32)).astype(bf)
        G[b, 0:CH] = h1
        cpy(h1s(b), h1p_h.at[r], hsem.at[b]).start()
        wide = h1.astype(f32)
        ya[1, r, :] = (wide * rms(wide)).astype(bf)
        acc[r, :] = jnp.zeros((CH, D), f32)
    each(0, T // CH, fin)
    for b in range(TWO): wt(h1s(0), hsem.at[b])
    def after(i):
        A3(i)
        A1(i + MATS)
    each(DEEP + TWO, DEEP + MATS, after)
    wt(dyp, dysem)

    def h1l(k): return cpy(h1p_h.at[pl.ds(k * D, D)], H.at[cut(D), pl.ds(k * D, D)], hsem.at[k])
    def abl(i): return cpy(AB_h.at[i], stv(i % MATS), stsem.at[i % MATS])
    def hload(j): return cpy(h_h.at[blk(j, TF), :], H.at[cut(TF)], hsem.at[TWO])
    def layer1(k, b):
        gu_wait(b)
        @pl.when(k + 1 < NT)
        def _(): gu_load(1, k + 1, 1 - b)
        def half(h):
            t = blk(h, TB)
            gu = dot_(wgu[b], ya[1, t, :], 0, 1)
            g, u = gu[:TF], gu[TF:]
            dh = dot_(wdb[blk(par(k), TF)], ya[0, t, :], 1, 1).astype(bf).astype(f32)
            sg = jax.nn.sigmoid(g)
            si = g * sg
            H[0:TF, t] = (si * u).astype(bf)
            H[TF2:TF3, t] = (dh * si).astype(bf)
            H[TF:TF2, t] = (dh * u * (sg + si * (1 - sg))).astype(bf)
            @pl.when(h == 0)
            def _(): guard(A2, k + DEEP + MATS)
        each(0, TWO, half)
        guard(A3, k + DEEP + MATS)
    def between():
        cpy(a0p_h, ap, asem).start()
        for k in range(TWO): wt(H.at[cut(D), cut(D)], hsem.at[k])
        def nb(i):
            r = blk(i, CH)
            wide = H[blk(ring(i), CH), blk(i // RING, D)].astype(f32)
            scale = rms(wide)
            da = acc[r, :].astype(bf).astype(f32)
            inner = jnp.mean(da * wide, -1, keepdims=True)
            dw = (da * scale - wide * (scale * scale * scale * inner)).astype(bf)
            ya[0, r, :] = (ya[0, r, :].astype(f32) + dw.astype(f32)).astype(bf)
        each(0, T // CH, nb)
        for i in range(TWO): abl(i).start()
        hload(0).start()
        wt(ap, asem)
    def layer0(j, b):
        def sub(s):
            i = j * RING + s
            @pl.when(i + TWO < NT * RING)
            def _(): abl(i + TWO).start()
            abl(i).wait()
            t, r = blk(s, TK), blk(i % MATS, TF)
            dh = dot_(wdb[blk(b, TF)], ya[0, t, :], 1, 1).astype(bf).astype(f32)
            H[TF2:TF3, t] = (dh * acc[r, 0:TK]).astype(bf)
            H[TF:TF2, t] = (dh * acc[r, TK:]).astype(bf)
        each(0, RING, sub)
        hload(j).wait()
    def tile(k):
        b, gb = par(k), par(k + 1)
        d_wait(b)
        @pl.when(k + 1 < NT)
        def _(): d_load(1, k + 1, 1 - b)
        @pl.when(jnp.logical_and(k + 1 >= NT, k + 1 < TWO * NT))
        def _(): d_load(0, k + 1 - NT, 1 - b)
        @pl.when(k < NT)
        def _(): layer1(k, gb)
        @pl.when(k == NT)
        def _(): between()
        @pl.when(k >= NT)
        def _(): layer0(k - NT, b)
        def mat(m):
            t = MATS * k + m
            slot(t)
            G[par(t)] = dot_(H[blk(m, TF)], ya[(m + 1) // TWO], 1, 0).astype(bf)
            S0(t)
            @pl.when(jnp.logical_and(k < NT, m < TWO))
            def _(): acc[blk(m, TB), :] += dot_(H[TF:TF3, blk(m, TB)], wgu[gb], 0, 1)
            @pl.when(jnp.logical_and(k == NT - 1, m == 1))
            def _():
                for q in range(TWO): h1l(q).start()
            @pl.when(jnp.logical_and(jnp.logical_and(k >= NT, k + 1 < TWO * NT), m == 0))
            def _(): hload(k - NT + 1).start()
        each(0, MATS, mat)
    each(0, TWO * NT, tile)
    each(NU, NU + TWO * len(STAGES), slot)

    SQ[me] = sqa[...]
    def sqc(e, i): return rd(sqa, SQ.at[i], sqs.at[e - 1], sqr.at[i], (0, r_, (me + e) % DEV))
    for e in range(1, DEV): sqc(e, me).start()
    def drain(n, k, sem): wt(GT.at[cut(n), cut(k)], sem)
    drain(NU - TWO * NT, TF, gtsem)
    drain(TWO, SH, locsem)
    drain(TWO * (DEV - 1), SH, a2s)
    for l in range(TWO): drain(DEV - 1, SH, a2r.at[l])
    for e in range(1, DEV):
        sqc(e, me).wait_send()
        sqc(e, (me + e) % DEV).wait_recv()
    tot = SQ[0]
    for i in range(1, DEV): tot = tot + SQ[i]
    sq_o[...] = tot


def train(x, dy, wg, wu, wd):
    hbm = pl.BlockSpec(memory_space=pl.ANY)
    V, S = pltpu.VMEM, pltpu.SemaphoreType.DMA
    b = (SUB, LANES)
    p3, r3, d3 = (TWO, TWO, MATS), (RING, TWO, MATS), (DEEP, TWO, MATS)
    one, two, three = S, S((TWO,)), S((MATS,))
    outs = [sds((NU, TF, LANES), bf), sds((TWO, SH, D), bf), sds((DEV, LANES), f32), sds((TWO, DEV, TWO, LANES, F), bf), sds((TWO, F, D), bf),
            sds((T, D), bf), sds((T, D), bf), sds((NT * RING, TF, D), f32), sds((F, T), bf)]
    specs = [hbm] * len(outs)
    specs[TWO] = pl.BlockSpec(memory_space=pltpu.VMEM)
    return pl.pallas_call(
        step_kernel,
        out_shape=outs, in_specs=[hbm] * (MATS + TWO), out_specs=specs,
        scratch_shapes=[
            V((TWO, T, D), bf), V((T, D), f32), V((TWO, D, TF2), bf), V((TF2, D), bf), V((TF3, T), bf), V((TWO, TF, D), bf), V((RING, TF, HALF), bf),
            V((TWO, TWO, RING, RING) + b, bf), V(r3 + (RING,) + b, bf), V((TWO, RING, TWO) + b, bf), V((RING, MATS, TWO) + b, bf), V((TWO, TWO) + b, bf), V((RING, TWO, RING) + b, bf),
            V((NU, TF, LANES), bf), V((DEV, LANES), f32), V((DEV, DEV, LANES), f32),
            one, one, one, two, two, three, three, S((RING,)), one, one,
            two, S((RING,)), S(p3), S(r3), S((TWO, MATS)), S((RING, MATS)), S(p3), S((RING, TWO, RING)), S(p3), S(r3), one, two,
            S(d3), S(d3), S((NA,)), S((NA,)), S(d3), S(d3), S((DEEP,)), S((NA,)), S((DEV - 1,)), S((DEV,))],
        compiler_params=pltpu.CompilerParams(collective_id=0, has_side_effects=True, vmem_limit_bytes=VMEM_LIMIT),
        name="train")(x, dy, wg, wu, wd)


def optimizer(sq, GT, GD, w, m, v):
    def kernel(sq, gg, gu, gd, *r):
        tot = jnp.sum(jnp.sum(sq[...], axis=0, keepdims=True), axis=1, keepdims=True)
        factor = jnp.minimum(1.0, 0.5 * lax.rsqrt(tot / (TWO * MATS * D * F) + 1e-30))
        ws, ms, vs, wo, mo, vo = (r[i * MATS:(i + 1) * MATS] for i in range(TWO * MATS))
        for i, block in enumerate((gg, gu, gd)):
            g = block[0].astype(f32)
            g = (g if i == TWO else g.T) * factor
            mm = 0.9 * ms[i][0] + 0.1 * g
            vv = 0.95 * vs[i][0] + 0.05 * g * g
            ww = ws[i][0].astype(f32)
            wo[i][0] = (ww - 0.02 * (mm * lax.rsqrt(vv + 1e-8) + 0.1 * ww)).astype(bf)
            mo[i][0], vo[i][0] = mm, vv
    def tile(i): return pl.BlockSpec((1, TF, LANES), lambda l, j: ((1 - l) * OFFLAY + MATS * j + i, 0, 0))
    a, d = pl.BlockSpec((1, LANES, TF), lambda l, j: (l, 0, j)), pl.BlockSpec((1, SUB, D), lambda l, j: (l, j, 0))
    outs = tuple(sds(q.shape, t) for t in (bf, f32, f32) for q in w)
    return pl.pallas_call(
        kernel, grid=(TWO, NT), in_specs=[pl.BlockSpec((DEV, LANES), lambda l, j: (0, 0)), tile(1), tile(TWO), d] + [a, a, d] * MATS,
        out_specs=(a, a, d) * MATS, out_shape=outs,
        compiler_params=pltpu.CompilerParams(vmem_limit_bytes=VMEM_LIMIT, dimension_semantics=("arbitrary",) * TWO),
        name="optimizer")(sq, GT, GT, GD, *w, *m, *v)


def solution(mesh):
    def step(x, dy, *arrays):
        w, m, v = (arrays[i:i + MATS] for i in range(0, len(arrays), MATS))
        GT, GD, sq = train(x[0], dy[0], *w)[:MATS]
        return optimizer(sq, GT, GD, w, m, v)
    states, cuts = P(("rep", "r", "s"), None, None), P(None, "s", None)
    return jax.shard_map(step, mesh=mesh, in_specs=(states, states) + (cuts,) * (MATS * MATS), out_specs=(P("rep", "s", None),) * (MATS * MATS), check_vma=False)
```

```python
import jax, jax.numpy as jnp
from jax import lax
from jax.experimental import pallas as pl
from jax.experimental.pallas import tpu as pltpu
from jax.sharding import PartitionSpec as P

bf, f32 = jnp.bfloat16, jnp.float32
T, D, F, TF = 2048, 1024, 3200, 640
TWO, MATS, RING = 2, 3, 4
NT = F // TF
NU = TWO * MATS * NT
NA = TWO * NT + TWO
DEEP = 6
LANES, SUB, HALF, CH, SH = 128, 80, 512, 256, 400
NCH = 2
DEV = D // LANES
TF2, TF3, TB = TWO * TF, MATS * TF, T // TWO
TC = TB // NCH
AROWS = LANES // DEV
OFFS = range(1, RING)
VMEM_LIMIT = 67043328
EPS = 1e-6
OFFLAY = NU // TWO


def sds(s, d): return jax.ShapeDtypeStruct(s, d)
def dot_(a, b, ca, cb): return lax.dot_general(a, b, (((ca,), (cb,)), ((), ())), preferred_element_type=f32)
def mul(i, n): return pl.multiple_of(i * n, n)
def blk(i, n): return pl.ds(mul(i, n), n)
def cut(n): return pl.ds(0, n)
def cpy(src, dst, sem): return pltpu.make_async_copy(src, dst, sem)
def wt(ref, sem): cpy(ref, ref, sem).wait()
def start(cs):
    for q in cs: q.start()
def each(lo, hi, f):
    def g(i, _):
        f(i)
        return _
    lax.fori_loop(lo, hi, g, 0)
def rms(wide): return lax.rsqrt(jnp.mean(wide * wide, -1, keepdims=True) + EPS)
def pc(k): return (k % TWO) * RING + k // TWO
def par(u): return u % TWO
def ring(u): return u % RING


def step_kernel(x_h, dy_h, wg_i, wu_i, wd_i,
                gt_o, gd_o, sq_o, WGU, WD, a0p_h, h1p_h, AB_h, h_h,
                ya, acc, wgu, wdb, H, G, R0, Pb, R1, Q, R2, U, R3, GT, sqa, SQ,
                dysem, asem, psem, ownsem, gusem, wdsem, stsem, hsem, gtsem, locsem,
                s0s, s0r, s1s, s1r, s2s, s2r, s3s, s3r, s4s, s4r, a2s, a2r,
                ag0s, ag0r, agds, agdr, ag1s, ag1r, ag2s, ag2r, sqs, sqr):
    r_, me = lax.axis_index("r"), lax.axis_index("s")
    x, y, z, c = me // TWO, r_ // RING, r_ % RING, me % TWO
    own = c * RING + x
    def dev(x, y, z, c): return (0, y * RING + z, x * TWO + c)
    def xdev(d): return dev(ring(x + d), y, z, c)
    def ydev(d): return dev(x, ring(y + d), z, c)
    def zdev(d): return dev(x, y, ring(z + d), c)
    part = dev(x, y, z, 1 - c)
    AX = ((0, y, ydev), (1, z, zdev))
    dyp, ap = ya.at[0], ya.at[1]
    bar = pltpu.get_barrier_semaphore()
    peers = [part] + [f(d) for f in (xdev, ydev, zdev) for d in OFFS] + [dev(ring(x + d), y, z, 1 - c) for d in OFFS]
    for p in peers: pl.semaphore_signal(bar, inc=1, device_id=p, device_id_type=pl.DeviceIdType.MESH)
    def rd(src, dst, ss, rs, d):
        return pltpu.make_async_remote_copy(src_ref=src, dst_ref=dst, send_sem=ss, recv_sem=rs, device_id=d, device_id_type=pl.DeviceIdType.MESH)
    def same(ref, ss, rs, d): return rd(ref, ref, ss, rs, d)
    def permuted(src, dst, sem): return [cpy(src.at[:, pl.ds(k * LANES, LANES)], dst.at[:, pl.ds(pc(k) * LANES, LANES)], sem) for k in range(DEV)]
    start(permuted(x_h, ap, psem))
    staged = [wdb.at[pl.ds(l * TF, SH)] for l in range(TWO)]
    for l in range(TWO): start(permuted(wd_i.at[l], staged[l], ownsem.at[l]))
    start(permuted(dy_h, dyp, dysem))
    sqa[...] = jnp.zeros_like(sqa)
    pl.semaphore_wait(bar, len(peers))

    def gu_load(l, j, b):
        for m, inp in enumerate((wg_i, wu_i)):
            cols = pl.ds(m * TF, TF)
            cpy(inp.at[l, :, blk(j, TF)], wgu.at[b, blk(own, LANES), cols], gusem.at[b]).start()
            def one(e):
                k = (own + e) % DEV
                cpy(WGU.at[l, k, m, :, blk(j, TF)], wgu.at[b, blk(k, LANES), cols], gusem.at[b]).start()
            each(1, DEV, one)
    def gu_wait(b): wt(wgu.at[b], gusem.at[b])
    def d_load(l, j, b): cpy(WD.at[l, blk(j, TF), :], wdb.at[blk(b, TF)], wdsem.at[b]).start()
    def d_wait(b): wt(wdb.at[blk(b, TF)], wdsem.at[b])

    def q16(h, q): return pl.ds(pl.multiple_of(h * (LANES // TWO) + q * AROWS, AROWS), AROWS)
    def colq(h, q): return blk(pc(RING * h + q), LANES)
    def fork(u, fg, fd):
        @pl.when(u % (NT + TWO) < NT)
        def _(): fg(u // (NT + TWO), u % (NT + TWO))
        @pl.when(u % (NT + TWO) >= NT)
        def _(): fd(u - NT)
    def wait6(ref, ss, rs, b):
        def one(i):
            h, d = i // MATS, i % MATS
            wt(ref, ss.at[b, h, d])
            wt(ref, rs.at[b, h, d])
        each(0, DEEP, one)
    def A0(u):
        b = u % DEEP
        def fg(l, j):
            for m, inp in enumerate((wg_i, wu_i)):
                def one(i):
                    for h, q, _ in AX: rd(inp.at[l, q16(h, q), blk(j, TF)], WGU.at[l, own, m, q16(h, q), blk(j, TF)], ag0s.at[b, h, i], ag0r.at[b, h, i], xdev(i + 1)).start()
                each(0, MATS, one)
                rd(inp.at[l, :, blk(j, TF)], WGU.at[l, own, m, :, blk(j, TF)], agds.at[u], agdr.at[u], part).start()
        def fd(l):
            wt(WD.at[0, cut(SH), :], ownsem.at[l])
            def one(i):
                for h, q, _ in AX: same(WD.at[l, blk(me, SH), colq(h, q)], ag0s.at[b, h, i], ag0r.at[b, h, i], xdev(i + 1)).start()
            each(0, MATS, one)
            same(WD.at[l, blk(me, SH), :], agds.at[u], agdr.at[u], part).start()
        fork(u, fg, fd)
    def A1(u):
        b = u % DEEP
        def fg(l, j):
            wait6(WGU.at[0, 0, :, cut(AROWS), cut(TF)], ag0s, ag0r, b)
            def one(i):
                k, d = c * RING + ring(x + i // MATS + 1), i % MATS
                for h, q, f in AX: same(WGU.at[l, k, :, q16(h, q), blk(j, TF)], ag1s.at[b, h, d], ag1r.at[b, h, d], f(d + 1)).start()
            each(0, MATS * MATS, one)
        def fd(l):
            wait6(WD.at[0, cut(SH), cut(LANES)], ag0s, ag0r, b)
            def one(i):
                k, d = TWO * ring(x + i // MATS + 1) + c, i % MATS
                for h, q, f in AX: same(WD.at[l, blk(k, SH), colq(h, q)], ag1s.at[b, h, d], ag1r.at[b, h, d], f(d + 1)).start()
            each(0, MATS * MATS, one)
        fork(u, fg, fd)
    gu1, gu3 = WGU.at[0, 0, :, :, cut(TF)], WGU.at[0, cut(MATS), :, :, cut(TF)]
    wd1, wd3 = WD.at[0, cut(SH), :], WD.at[0, cut(MATS * SH), :]
    def A2(u):
        b = u % DEEP
        def fg(l, j):
            wait6(WGU.at[0, cut(MATS), :, cut(AROWS), cut(TF)], ag1s, ag1r, b)
            each(1, RING, lambda i: same(WGU.at[l, c * RING + ring(x + i), :, :, blk(j, TF)], ag2s.at[b], ag2r.at[u], part).start())
        def fd(l):
            wait6(WD.at[0, cut(MATS * SH), cut(LANES)], ag1s, ag1r, b)
            each(1, RING, lambda i: same(WD.at[l, blk(TWO * ring(x + i) + c, SH), :], ag2s.at[b], ag2r.at[u], part).start())
        fork(u, fg, fd)
    def A3(u):
        b = u % DEEP
        def done(one, three):
            for ref, sem in ((one, agds.at[u]), (one, agdr.at[u]), (three, ag2s.at[b]), (three, ag2r.at[u])): wt(ref, sem)
        fork(u, lambda l, j: done(gu1, gu3), lambda l: done(wd1, wd3))
    def guard(A, u):
        @pl.when(jnp.logical_and(u >= 0, u < NA))
        def _(): A(u)

    def c0(u): return rd(G.at[par(u), :, blk(1 - c, HALF)], R0.at[ring(u)], s0s.at[par(u)], s0r.at[ring(u)], part)
    def mat_(u): return u % MATS
    def deep(u): return u % DEEP
    def c1(u):
        return [rd(Pb.at[mat_(u), h, ring(q + d)], R1.at[ring(u), h, d - 1], s1s.at[ring(u), h, d - 1], s1r.at[ring(u), h, d - 1], f(d)) for d in OFFS for h, q, f in AX]
    def c1x(u): return [rd(Pb.at[mat_(u), :, :, ring(x + d)], R1.at[ring(u), :, d - 1], s1s.at[ring(u), 0, d - 1], s1r.at[ring(u), 0, d - 1], xdev(d)) for d in OFFS]
    def c2(u): return [rd(Q.at[par(u), ring(x + d)], R2.at[deep(u), d - 1], s2s.at[par(u), 0, d - 1], s2r.at[deep(u), 0, d - 1], xdev(d)) for d in OFFS]
    def c2x(u):
        return [rd(Q.at[par(u), ring(q + d), h], R2.at[deep(u), d - 1, h], s2s.at[par(u), h, d - 1], s2r.at[deep(u), h, d - 1], f(d)) for d in OFFS for h, q, f in AX]
    def either(u, f, *args):
        @pl.when(mat_(u) > 0)
        def _(): f(*args[0])
        @pl.when(mat_(u) == 0)
        def _(): f(*args[1])
    def c3(u, recv):
        o = []
        for d in OFFS:
            for h, q, f in ((0, z, zdev), (1, y, ydev)):
                k = ring(q + d) if recv else q
                o.append(rd(U.at[par(u), h], R3.at[ring(u), h, k], s3s.at[par(u), h, d - 1], s3r.at[ring(u), h, k], f(d)))
        return o
    def rows(h, q): return pl.ds(pl.multiple_of(h * (TF // TWO) + q * SUB, SUB), SUB)
    def c4(u):
        return [same(GT.at[u, rows(h, q)], s4s.at[par(u), h, d - 1], s4r.at[ring(u), h, d - 1], f(d)) for d in OFFS for h, q, f in AX]
    def S0(u): c0(u).start()
    def S1(u):
        c0(u).wait()
        def one(i):
            for k in range(RING):
                mine = G[par(u), blk(i, SUB), blk(c * RING + k, LANES)]
                Pb[mat_(u), i // RING, ring(i), k] = (mine.astype(f32) + R0[ring(u), blk(i, SUB), pl.ds(k * LANES, LANES)].astype(f32)).astype(bf)
        each(0, DEV, one)
        either(u, lambda way: start(way(u)), (c1,), (c1x,))
    def added(first, rest):
        s = first.astype(f32)
        for q in rest: s = s + q.astype(f32)
        return s.astype(bf)
    def second(u, got, first, send):
        for q in got(u): q.wait()
        for h, mine, _ in AX:
            for k in range(RING): Q[par(u), k, h] = added(first(h, mine, k), [R1[ring(u), h, d, k] for d in range(MATS)])
        start(send(u))
    def S2(u):
        @pl.when(mat_(u) > 0)
        def _(): second(u, c1, lambda h, mine, k: Pb[mat_(u), h, mine, k], c2)
    def S2x(u):
        @pl.when(mat_(u) == 0)
        def _(): second(u, c1x, lambda h, mine, k: Pb[mat_(u), h, k, x], c2x)
    def S3(u):
        def go(got, mine):
            for q in got(u): q.wait()
            for h in range(TWO): U[par(u), h] = added(Q[par(u), mine[h], h], [R2[deep(u), d, h] for d in range(MATS)])
        either(u, go, (c2, (x, x)), (c2x, (y, z)))
        start(c3(u, False))
    def S4(u):
        for q in c3(u, False): q.wait_send()
        for q in c3(u, True): q.wait_recv()
        R3[ring(u), 0, z] = U[par(u), 0]
        R3[ring(u), 1, y] = U[par(u), 1]
        for h, q, _ in AX:
            s = R3[ring(u), h, 0].astype(f32)
            for d in OFFS: s = s + R3[ring(u), h, d].astype(f32)
            GT[u, rows(h, q)] = s.astype(bf)
        start(c4(u))
    def a2a(u, i):
        lay, n = u // OFFLAY, DEV * ((u % OFFLAY) // MATS) + i
        to = n // NT
        src, dst = GT.at[u, blk(i, SUB)], gd_o.at[1 - lay, blk(n - NT * to, SUB), blk(me, LANES)]
        @pl.when(to != me)
        def _(): rd(src, dst, a2s, a2r.at[lay], (0, r_, to)).start()
        @pl.when(to == me)
        def _(): cpy(src, dst, locsem).start()
    def S5(u):
        for q in c4(u): q.wait()
        v = GT[u].astype(f32)
        sqa[...] += jnp.sum((v * v).reshape(SUB, DEV, LANES), axis=0)
        @pl.when(u % MATS > 0)
        def _(): cpy(GT.at[u], gt_o.at[u], gtsem).start()
        @pl.when(u % MATS == 0)
        def _():
            each(0, DEV, lambda i: a2a(u, i))
    LAST = TWO * len((S1, S2, S3, S4, S5))
    STAGES = ((S5, LAST), (S4, LAST - TWO), (S3, LAST - RING), (S2, RING), (S2x, NT), (S1, TWO))
    def slot(t):
        for S, lag in STAGES:
            @pl.when(jnp.logical_and(t >= lag, t < NU + lag))
            def _(): S(t - lag)

    each(0, MATS, A0)
    for l in range(TWO):
        wt(staged[l], ownsem.at[l])
        cpy(staged[l], WD.at[l, blk(me, SH), :], ownsem.at[l]).start()
    wt(ap, psem)
    def xnorm(i):
        wide = ya[1, blk(i, CH), :].astype(f32)
        ya[1, blk(i, CH), :] = (wide * rms(wide)).astype(bf)
    each(0, T // CH, xnorm)
    cpy(ap, a0p_h, asem).start()
    def head(i):
        guard(A2, i - 1)
        @pl.when(i == 0)
        def _(): A1(i)
        A1(i + 1)
        A0(i + MATS)
    each(0, TWO, head)
    each(0, 1, A3)
    gu_load(0, 0, 0)
    each(MATS, RING, A1)
    each(NT, DEEP, A0)
    def stv(i): return acc.at[blk(i, TF2), :]
    def step1(j):
        b = par(j)
        gu_wait(b)
        hs = j % MATS
        hr = blk(hs, TF)
        @pl.when(j >= MATS)
        def _(): wt(H.at[cut(TF)], hsem.at[hs])
        @pl.when(j > 0)
        def _(): guard(A2, j + 1)
        def sub(s):
            @pl.when(j > 0)
            def _(): wt(stv(0), stsem.at[s])
            for q in range(NCH):
                t, cols = pl.ds(pl.multiple_of(s * TB + q * TC, TC), TC), pl.ds(q * TC, TC)
                gu = dot_(wgu[b], ya[1, t, :], 0, 1)
                g, u = gu[:TF], gu[TF:]
                sg = jax.nn.sigmoid(g)
                si = g * sg
                acc[pl.ds(mul(s, TF2), TF), cols] = si
                acc[pl.ds(pl.multiple_of(s * TF2 + TF, TF), TF), cols] = u * (sg + si * (1 - sg))
                H[hr, t] = (si * u).astype(bf)
            cpy(stv(s), AB_h.at[TWO * j + s], stsem.at[s]).start()
            @pl.when(s == 0)
            def _():
                @pl.when(j == 0)
                def _(): A2(j + 1)
                guard(A3, j + 1)
                @pl.when(j < NT - 1)
                def _(): gu_load(0, j + 1, 1 - b)
                @pl.when(j == NT - 1)
                def _(): cpy(WD.at[0, pl.ds(TF3, TF2), :], wdb, wdsem.at[TWO]).start()
                guard(A1, j + RING)
                guard(A0, j + DEEP)
        each(0, TWO, sub)
        cpy(H.at[hr], h_h.at[blk(j, TF), :], hsem.at[hs]).start()
    each(0, NT, step1)
    for i in range(TWO): wt(stv(0), stsem.at[i])
    wt(ap, asem)
    start(permuted(x_h, ap, psem))
    lo, mid = cut(TF2), wgu.at[0, cut(TF), cut(D)]
    cpy(WD.at[0, pl.ds(TF2, TF), :], mid, wdsem.at[0]).start()
    acc[0:T, :] = jnp.zeros((T, D), f32)
    def down(i):
        @pl.when(i == 1)
        def _(): wt(H.at[lo], hsem.at[MATS])
        wt(wdb, wdsem.at[TWO])
        def halves(h): acc[blk(h, TB), :] += dot_(H[lo, blk(h, TB)], wdb[...], 0, 0)
        each(0, TWO, halves)
        @pl.when(i == 0)
        def _():
            for k in range(TWO): wt(H.at[cut(TF)], hsem.at[k])
            cpy(h_h.at[lo], H.at[lo], hsem.at[MATS]).start()
            cpy(WD.at[0, lo, :], wdb, wdsem.at[TWO]).start()
            A2(i + DEEP)
            A1(i + NA - MATS)
            A0(i + NA - 1)
            wt(mid, wdsem.at[0])
            def halves(h): acc[blk(h, TB), :] += dot_(H[TF2:TF3, blk(h, TB)], wgu[0, 0:TF, 0:D], 0, 0)
            each(0, TWO, halves)
        A3(i + DEEP)
        A2(i + DEEP + 1)
        @pl.when(i == 0)
        def _(): A1(i + NA - TWO)
    each(0, TWO, down)
    gu_load(1, 0, 1)
    d_load(1, 0, 0)
    wt(H.at[cut(TF)], hsem.at[TWO])
    wt(ap, psem)
    def h1s(b): return G.at[b, cut(CH)]
    def fin(i):
        b, r = par(i), blk(i, CH)
        @pl.when(i >= TWO)
        def _(): wt(h1s(0), hsem.at[b])
        h1 = (ya[1, r, :].astype(f32) + acc[r, :].astype(bf).astype(f32)).astype(bf)
        G[b, 0:CH] = h1
        cpy(h1s(b), h1p_h.at[r], hsem.at[b]).start()
        wide = h1.astype(f32)
        ya[1, r, :] = (wide * rms(wide)).astype(bf)
        acc[r, :] = jnp.zeros((CH, D), f32)
    each(0, T // CH, fin)
    for b in range(TWO): wt(h1s(0), hsem.at[b])
    def after(i):
        A3(i)
        A1(i + MATS)
    each(DEEP + TWO, DEEP + MATS, after)
    wt(dyp, dysem)

    def h1l(k): return cpy(h1p_h.at[pl.ds(k * D, D)], H.at[cut(D), pl.ds(k * D, D)], hsem.at[k])
    def abl(j, s): return cpy(AB_h.at[TWO * j + s], stv(s), stsem.at[s])
    def hload(j): return cpy(h_h.at[blk(j, TF), :], H.at[cut(TF)], hsem.at[TWO])
    def layer1(k, b):
        gu_wait(b)
        @pl.when(k + 1 < NT)
        def _(): gu_load(1, k + 1, 1 - b)
        def half(h):
            for q in range(NCH):
                t = pl.ds(pl.multiple_of(h * TB + q * TC, TC), TC)
                gu = dot_(wgu[b], ya[1, t, :], 0, 1)
                g, u = gu[:TF], gu[TF:]
                dh = dot_(wdb[blk(par(k), TF)], ya[0, t, :], 1, 1).astype(bf).astype(f32)
                sg = jax.nn.sigmoid(g)
                si = g * sg
                H[0:TF, t] = (si * u).astype(bf)
                H[TF2:TF3, t] = (dh * si).astype(bf)
                H[TF:TF2, t] = (dh * u * (sg + si * (1 - sg))).astype(bf)
            @pl.when(h == 0)
            def _(): guard(A2, k + DEEP + MATS)
        each(0, TWO, half)
        guard(A3, k + DEEP + MATS)
    def between():
        cpy(a0p_h, ap, asem).start()
        for k in range(TWO): wt(H.at[cut(D), cut(D)], hsem.at[k])
        def nb(i):
            r = blk(i, CH)
            wide = H[blk(ring(i), CH), blk(i // RING, D)].astype(f32)
            scale = rms(wide)
            da = acc[r, :].astype(bf).astype(f32)
            inner = jnp.mean(da * wide, -1, keepdims=True)
            dw = (da * scale - wide * (scale * scale * scale * inner)).astype(bf)
            ya[0, r, :] = (ya[0, r, :].astype(f32) + dw.astype(f32)).astype(bf)
            @pl.when(i == TF2 // CH - 1)
            def _(): abl(0, 0).start()
        each(0, T // CH, nb)
        abl(0, 1).start()
        hload(0).start()
        wt(ap, asem)
    def layer0(j, b):
        def sub(s):
            abl(j, s).wait()
            for q in range(NCH):
                t, cols = pl.ds(pl.multiple_of(s * TB + q * TC, TC), TC), pl.ds(q * TC, TC)
                dh = dot_(wdb[blk(b, TF)], ya[0, t, :], 1, 1).astype(bf).astype(f32)
                H[TF2:TF3, t] = (dh * acc[pl.ds(mul(s, TF2), TF), cols]).astype(bf)
                H[TF:TF2, t] = (dh * acc[pl.ds(pl.multiple_of(s * TF2 + TF, TF), TF), cols]).astype(bf)
            @pl.when(j + 1 < NT)
            def _(): abl(j + 1, s).start()
        each(0, TWO, sub)
        hload(j).wait()
    def tile(k):
        b, gb = par(k), par(k + 1)
        d_wait(b)
        @pl.when(k + 1 < NT)
        def _(): d_load(1, k + 1, 1 - b)
        @pl.when(jnp.logical_and(k + 1 >= NT, k + 1 < TWO * NT))
        def _(): d_load(0, k + 1 - NT, 1 - b)
        @pl.when(k < NT)
        def _(): layer1(k, gb)
        @pl.when(k == NT)
        def _(): between()
        @pl.when(k >= NT)
        def _(): layer0(k - NT, b)
        def mat(m):
            t = MATS * k + m
            slot(t)
            G[par(t)] = dot_(H[blk(m, TF)], ya[(m + 1) // TWO], 1, 0).astype(bf)
            S0(t)
            @pl.when(jnp.logical_and(k < NT, m < TWO))
            def _(): acc[blk(m, TB), :] += dot_(H[TF:TF3, blk(m, TB)], wgu[gb], 0, 1)
            @pl.when(jnp.logical_and(k == NT - 1, m == 1))
            def _():
                for q in range(TWO): h1l(q).start()
            @pl.when(jnp.logical_and(jnp.logical_and(k >= NT, k + 1 < TWO * NT), m == 0))
            def _(): hload(k - NT + 1).start()
        each(0, MATS, mat)
    each(0, TWO * NT, tile)
    each(NU, NU + LAST, slot)

    SQ[me] = sqa[...]
    def sqc(e, i): return rd(sqa, SQ.at[i], sqs.at[e - 1], sqr.at[i], (0, r_, (me + e) % DEV))
    for e in range(1, DEV): sqc(e, me).start()
    def drain(n, k, sem): wt(GT.at[cut(n), cut(k)], sem)
    drain(NU - TWO * NT, TF, gtsem)
    drain(TWO, SH, locsem)
    drain(TWO * (DEV - 1), SH, a2s)
    for l in range(TWO): drain(DEV - 1, SH, a2r.at[l])
    for e in range(1, DEV):
        sqc(e, me).wait_send()
        sqc(e, (me + e) % DEV).wait_recv()
    tot = SQ[0]
    for i in range(1, DEV): tot = tot + SQ[i]
    sq_o[...] = tot


def train(x, dy, wg, wu, wd):
    hbm = pl.BlockSpec(memory_space=pl.ANY)
    V, S = pltpu.VMEM, pltpu.SemaphoreType.DMA
    b = (SUB, LANES)
    p3, r3, d3 = (TWO, TWO, MATS), (RING, TWO, MATS), (DEEP, TWO, MATS)
    one, two, three = S, S((TWO,)), S((MATS,))
    outs = [sds((NU, TF, LANES), bf), sds((TWO, SH, D), bf), sds((DEV, LANES), f32), sds((TWO, DEV, TWO, LANES, F), bf), sds((TWO, F, D), bf),
            sds((T, D), bf), sds((T, D), bf), sds((NT * TWO, TF2, D), f32), sds((F, T), bf)]
    specs = [hbm] * len(outs)
    specs[TWO] = pl.BlockSpec(memory_space=pltpu.VMEM)
    return pl.pallas_call(
        step_kernel,
        out_shape=outs, in_specs=[hbm] * (MATS + TWO), out_specs=specs,
        scratch_shapes=[
            V((TWO, T, D), bf), V((TWO * TF2, D), f32), V((TWO, D, TF2), bf), V((TF2, D), bf), V((TF3, T), bf), V((TWO, TF, D), bf), V((RING, TF, HALF), bf),
            V((MATS, TWO, RING, RING) + b, bf), V(r3 + (RING,) + b, bf), V((TWO, RING, TWO) + b, bf), V((DEEP, MATS, TWO) + b, bf), V((TWO, TWO) + b, bf), V((RING, TWO, RING) + b, bf),
            V((NU, TF, LANES), bf), V((DEV, LANES), f32), V((DEV, DEV, LANES), f32),
            one, one, one, two, two, three, two, S((RING,)), one, one,
            two, S((RING,)), S(r3), S(r3), S(p3), S(d3), S(p3), S((RING, TWO, RING)), S(p3), S(r3), one, two,
            S(d3), S(d3), S((NA,)), S((NA,)), S(d3), S(d3), S((DEEP,)), S((NA,)), S((DEV - 1,)), S((DEV,))],
        compiler_params=pltpu.CompilerParams(collective_id=0, has_side_effects=True, vmem_limit_bytes=VMEM_LIMIT),
        name="train")(x, dy, wg, wu, wd)


def optimizer(sq, GT, GD, w, m, v):
    def kernel(sq, gg, gu, gd, *r):
        tot = jnp.sum(jnp.sum(sq[...], axis=0, keepdims=True), axis=1, keepdims=True)
        factor = jnp.minimum(1.0, 0.5 * lax.rsqrt(tot / (TWO * MATS * D * F) + 1e-30))
        ws, ms, vs, wo, mo, vo = (r[i * MATS:(i + 1) * MATS] for i in range(TWO * MATS))
        for i, block in enumerate((gg, gu, gd)):
            g = block[0].astype(f32)
            g = (g if i == TWO else g.T) * factor
            mm = 0.9 * ms[i][0] + 0.1 * g
            vv = 0.95 * vs[i][0] + 0.05 * g * g
            ww = ws[i][0].astype(f32)
            wo[i][0] = (ww - 0.02 * (mm * lax.rsqrt(vv + 1e-8) + 0.1 * ww)).astype(bf)
            mo[i][0], vo[i][0] = mm, vv
    def tile(i): return pl.BlockSpec((1, TF, LANES), lambda l, j: ((1 - l) * OFFLAY + MATS * j + i, 0, 0))
    a, d = pl.BlockSpec((1, LANES, TF), lambda l, j: (l, 0, j)), pl.BlockSpec((1, SUB, D), lambda l, j: (l, j, 0))
    outs = tuple(sds(q.shape, t) for t in (bf, f32, f32) for q in w)
    return pl.pallas_call(
        kernel, grid=(TWO, NT), in_specs=[pl.BlockSpec((DEV, LANES), lambda l, j: (0, 0)), tile(1), tile(TWO), d] + [a, a, d] * MATS,
        out_specs=(a, a, d) * MATS, out_shape=outs,
        compiler_params=pltpu.CompilerParams(vmem_limit_bytes=VMEM_LIMIT, dimension_semantics=("arbitrary",) * TWO),
        name="optimizer")(sq, GT, GT, GD, *w, *m, *v)


def solution(mesh):
    def step(x, dy, *arrays):
        w, m, v = (arrays[i:i + MATS] for i in range(0, len(arrays), MATS))
        GT, GD, sq = train(x[0], dy[0], *w)[:MATS]
        return optimizer(sq, GT, GD, w, m, v)
    states, cuts = P(("rep", "r", "s"), None, None), P(None, "s", None)
    return jax.shard_map(step, mesh=mesh, in_specs=(states, states) + (cuts,) * (MATS * MATS), out_specs=(P("rep", "s", None),) * (MATS * MATS), check_vma=False)
```

```python
import jax, jax.numpy as jnp
from jax import lax
from jax.experimental import pallas as pl
from jax.experimental.pallas import tpu as pltpu
from jax.sharding import PartitionSpec as P

bf, f32 = jnp.bfloat16, jnp.float32
T, D, F, TF = 2048, 1024, 3200, 640
TWO, MATS, RING = 2, 3, 4
NT = F // TF
NU = TWO * MATS * NT
NA = TWO * NT + TWO
DEEP = 6
LANES, SUB, HALF, CH, SH = 128, 80, 512, 256, 400
NCH = 2
DEV = D // LANES
TF2, TF3, TB = TWO * TF, MATS * TF, T // TWO
TC = TB // NCH
AROWS = LANES // DEV
OFFS = range(1, RING)
VMEM_LIMIT = 67043328
EPS = 1e-6
OFFLAY = NU // TWO


def sds(s, d): return jax.ShapeDtypeStruct(s, d)
def dot_(a, b, ca, cb): return lax.dot_general(a, b, (((ca,), (cb,)), ((), ())), preferred_element_type=f32)
def mul(i, n): return pl.multiple_of(i * n, n)
def blk(i, n): return pl.ds(mul(i, n), n)
def cut(n): return pl.ds(0, n)
def cpy(src, dst, sem): return pltpu.make_async_copy(src, dst, sem)
def wt(ref, sem): cpy(ref, ref, sem).wait()
def start(cs):
    for q in cs: q.start()
def each(lo, hi, f):
    def g(i, _):
        f(i)
        return _
    lax.fori_loop(lo, hi, g, 0)
def rms(wide): return lax.rsqrt(jnp.mean(wide * wide, -1, keepdims=True) + EPS)
def pc(k): return (k % TWO) * RING + k // TWO
def par(u): return u % TWO
def ring(u): return u % RING


def step_kernel(x_h, dy_h, wg_i, wu_i, wd_i,
                gt_o, gd_o, sq_o, WGU, WD, a0p_h, h1p_h, AB_h, h_h,
                ya, acc, wgu, wdb, H, G, R0, Pb, R1, Q, R2, U, R3, GT, sqa, SQ,
                dysem, asem, psem, ownsem, gusem, wdsem, stsem, hsem, gtsem, locsem,
                s0s, s0r, s1s, s1r, s2s, s2r, s3s, s3r, s4s, s4r, a2s, a2r,
                ag0s, ag0r, agds, agdr, ag1s, ag1r, ag2s, ag2r, sqs, sqr):
    r_, me = lax.axis_index("r"), lax.axis_index("s")
    x, y, z, c = me // TWO, r_ // RING, r_ % RING, me % TWO
    own = c * RING + x
    def dev(x, y, z, c): return (0, y * RING + z, x * TWO + c)
    def xdev(d): return dev(ring(x + d), y, z, c)
    def ydev(d): return dev(x, ring(y + d), z, c)
    def zdev(d): return dev(x, y, ring(z + d), c)
    part = dev(x, y, z, 1 - c)
    AX = ((0, y, ydev), (1, z, zdev))
    dyp, ap = ya.at[0], ya.at[1]
    bar = pltpu.get_barrier_semaphore()
    peers = [part] + [f(d) for f in (xdev, ydev, zdev) for d in OFFS] + [dev(ring(x + d), y, z, 1 - c) for d in OFFS]
    for p in peers: pl.semaphore_signal(bar, inc=1, device_id=p, device_id_type=pl.DeviceIdType.MESH)
    def rd(src, dst, ss, rs, d):
        return pltpu.make_async_remote_copy(src_ref=src, dst_ref=dst, send_sem=ss, recv_sem=rs, device_id=d, device_id_type=pl.DeviceIdType.MESH)
    def same(ref, ss, rs, d): return rd(ref, ref, ss, rs, d)
    def permuted(src, dst, sem): return [cpy(src.at[:, pl.ds(k * LANES, LANES)], dst.at[:, pl.ds(pc(k) * LANES, LANES)], sem) for k in range(DEV)]
    start(permuted(x_h, ap, psem))
    staged = [wdb.at[pl.ds(l * TF, SH)] for l in range(TWO)]
    for l in range(TWO): start(permuted(wd_i.at[l], staged[l], ownsem.at[l]))
    start(permuted(dy_h, dyp, dysem))
    sqa[...] = jnp.zeros_like(sqa)
    pl.semaphore_wait(bar, len(peers))

    def gu_load(l, j, b):
        for m, inp in enumerate((wg_i, wu_i)):
            cols = pl.ds(m * TF, TF)
            cpy(inp.at[l, :, blk(j, TF)], wgu.at[b, blk(own, LANES), cols], gusem.at[b]).start()
            def one(e):
                k = (own + e) % DEV
                cpy(WGU.at[l, k, m, :, blk(j, TF)], wgu.at[b, blk(k, LANES), cols], gusem.at[b]).start()
            each(1, DEV, one)
    def gu_wait(b): wt(wgu.at[b], gusem.at[b])
    def d_load(l, j, b): cpy(WD.at[l, blk(j, TF), :], wdb.at[blk(b, TF)], wdsem.at[b]).start()
    def d_wait(b): wt(wdb.at[blk(b, TF)], wdsem.at[b])

    def q16(h, q): return pl.ds(pl.multiple_of(h * (LANES // TWO) + q * AROWS, AROWS), AROWS)
    def colq(h, q): return blk(pc(RING * h + q), LANES)
    def fork(u, fg, fd):
        @pl.when(u % (NT + TWO) < NT)
        def _(): fg(u // (NT + TWO), u % (NT + TWO))
        @pl.when(u % (NT + TWO) >= NT)
        def _(): fd(u - NT)
    def both(ref, ss, rs, b):
        wt(ref, ss.at[b])
        wt(ref, rs.at[b])
    def A0(u):
        b = u % DEEP
        def fg(l, j):
            for m, inp in enumerate((wg_i, wu_i)):
                def one(i):
                    for h, q, _ in AX: rd(inp.at[l, q16(h, q), blk(j, TF)], WGU.at[l, own, m, q16(h, q), blk(j, TF)], ag0s.at[b], ag0r.at[b], xdev(i + 1)).start()
                each(0, MATS, one)
                rd(inp.at[l, :, blk(j, TF)], WGU.at[l, own, m, :, blk(j, TF)], agds.at[u], agdr.at[u], part).start()
        def fd(l):
            wt(WD.at[0, cut(SH), :], ownsem.at[l])
            def one(i):
                for h, q, _ in AX: same(WD.at[l, blk(me, SH), colq(h, q)], ag0s.at[b], ag0r.at[b], xdev(i + 1)).start()
            each(0, MATS, one)
            same(WD.at[l, blk(me, SH), :], agds.at[u], agdr.at[u], part).start()
        fork(u, fg, fd)
    def A1(u):
        b = u % DEEP
        def fg(l, j):
            both(WGU.at[0, cut(DEEP), :, cut(AROWS), cut(TF)], ag0s, ag0r, b)
            def one(i):
                k, d = c * RING + ring(x + i // MATS + 1), i % MATS
                for h, q, f in AX: same(WGU.at[l, k, :, q16(h, q), blk(j, TF)], ag1s.at[b], ag1r.at[b], f(d + 1)).start()
            each(0, MATS * MATS, one)
        def fd(l):
            both(WD.at[0, cut(DEEP * SH), cut(LANES)], ag0s, ag0r, b)
            def one(i):
                k, d = TWO * ring(x + i // MATS + 1) + c, i % MATS
                for h, q, f in AX: same(WD.at[l, blk(k, SH), colq(h, q)], ag1s.at[b], ag1r.at[b], f(d + 1)).start()
            each(0, MATS * MATS, one)
        fork(u, fg, fd)
    gu1, gu3 = WGU.at[0, 0, :, :, cut(TF)], WGU.at[0, cut(MATS), :, :, cut(TF)]
    wd1, wd3 = WD.at[0, cut(SH), :], WD.at[0, cut(MATS * SH), :]
    def A2(u):
        b = u % DEEP
        def fg(l, j):
            both(WGU.at[0, cut(DEEP), :, cut(MATS * AROWS), cut(TF)], ag1s, ag1r, b)
            each(1, RING, lambda i: same(WGU.at[l, c * RING + ring(x + i), :, :, blk(j, TF)], ag2s.at[b], ag2r.at[u], part).start())
        def fd(l):
            both(WD.at[0, cut(DEEP * SH), cut(MATS * LANES)], ag1s, ag1r, b)
            each(1, RING, lambda i: same(WD.at[l, blk(TWO * ring(x + i) + c, SH), :], ag2s.at[b], ag2r.at[u], part).start())
        fork(u, fg, fd)
    def A3(u):
        b = u % DEEP
        def done(one, three):
            for ref, sem in ((one, agds.at[u]), (one, agdr.at[u]), (three, ag2s.at[b]), (three, ag2r.at[u])): wt(ref, sem)
        fork(u, lambda l, j: done(gu1, gu3), lambda l: done(wd1, wd3))
    def guard(A, u):
        @pl.when(jnp.logical_and(u >= 0, u < NA))
        def _(): A(u)

    def c0(u): return rd(G.at[par(u), :, blk(1 - c, HALF)], R0.at[ring(u)], s0s.at[par(u)], s0r.at[ring(u)], part)
    def mat_(u): return u % MATS
    def deep(u): return u % DEEP
    def c1(u):
        return [rd(Pb.at[mat_(u), h, ring(q + d)], R1.at[ring(u), h, d - 1], s1s.at[ring(u)], s1r.at[ring(u)], f(d)) for d in OFFS for h, q, f in AX]
    def c1x(u): return [rd(Pb.at[mat_(u), :, :, ring(x + d)], R1.at[ring(u), :, d - 1], s1s.at[ring(u)], s1r.at[ring(u)], xdev(d)) for d in OFFS]
    def c2(u): return [rd(Q.at[par(u), ring(x + d)], R2.at[deep(u), d - 1], s2s.at[par(u)], s2r.at[deep(u)], xdev(d)) for d in OFFS]
    def c2x(u):
        return [rd(Q.at[par(u), ring(q + d), h], R2.at[deep(u), d - 1, h], s2s.at[par(u)], s2r.at[deep(u)], f(d)) for d in OFFS for h, q, f in AX]
    def either(u, f, *args):
        @pl.when(mat_(u) > 0)
        def _(): f(*args[0])
        @pl.when(mat_(u) == 0)
        def _(): f(*args[1])
    def c3(u):
        return [rd(U.at[par(u), h], R3.at[ring(u), h, q], s3s.at[par(u)], s3r.at[ring(u)], f(d)) for d in OFFS for h, q, f in ((0, z, zdev), (1, y, ydev))]
    def rows(h, q): return pl.ds(pl.multiple_of(h * (TF // TWO) + q * SUB, SUB), SUB)
    def c4(u):
        return [same(GT.at[u, rows(h, q)], s4s.at[par(u)], s4r.at[ring(u)], f(d)) for d in OFFS for h, q, f in AX]
    def S0(u): c0(u).start()
    def S1(u):
        c0(u).wait()
        for i in range(DEV):
            for k in range(RING):
                mine = G[par(u), pl.ds(i * SUB, SUB), blk(c * RING + k, LANES)]
                Pb[mat_(u), i // RING, i % RING, k] = (mine.astype(f32) + R0[ring(u), pl.ds(i * SUB, SUB), pl.ds(k * LANES, LANES)].astype(f32)).astype(bf)
        either(u, lambda way: start(way(u)), (c1,), (c1x,))
    def added(first, rest):
        s = first.astype(f32)
        for q in rest: s = s + q.astype(f32)
        return s.astype(bf)
    def second(u, first, send):
        wt(R1.at[0], s1s.at[ring(u)])
        wt(R1.at[0], s1r.at[ring(u)])
        for h, mine, _ in AX:
            for k in range(RING): Q[par(u), k, h] = added(first(h, mine, k), [R1[ring(u), h, d, k] for d in range(MATS)])
        start(send(u))
    def S2(u):
        @pl.when(mat_(u) > 0)
        def _(): second(u, lambda h, mine, k: Pb[mat_(u), h, mine, k], c2)
    def S2x(u):
        @pl.when(mat_(u) == 0)
        def _(): second(u, lambda h, mine, k: Pb[mat_(u), h, k, x], c2x)
    def S3(u):
        wt(R2.at[0], s2s.at[par(u)])
        wt(R2.at[0], s2r.at[deep(u)])
        def go(*mine):
            for h in range(TWO): U[par(u), h] = added(Q[par(u), mine[h], h], [R2[deep(u), d, h] for d in range(MATS)])
        either(u, go, (x, x), (y, z))
        start(c3(u))
    def S4(u):
        wt(R2.at[0], s3s.at[par(u)])
        wt(R2.at[0], s3r.at[ring(u)])
        R3[ring(u), 0, z] = U[par(u), 0]
        R3[ring(u), 1, y] = U[par(u), 1]
        for h, q, _ in AX:
            s = R3[ring(u), h, 0].astype(f32)
            for d in OFFS: s = s + R3[ring(u), h, d].astype(f32)
            GT[u, rows(h, q)] = s.astype(bf)
        start(c4(u))
    def a2a(u, i):
        lay, n = u // OFFLAY, DEV * ((u % OFFLAY) // MATS) + i
        to = n // NT
        src, dst = GT.at[u, blk(i, SUB)], gd_o.at[1 - lay, blk(n - NT * to, SUB), blk(me, LANES)]
        @pl.when(to != me)
        def _(): rd(src, dst, a2s, a2r.at[lay], (0, r_, to)).start()
        @pl.when(to == me)
        def _(): cpy(src, dst, locsem).start()
    def S5(u):
        wt(R2.at[0], s4s.at[par(u)])
        wt(R2.at[0], s4r.at[ring(u)])
        v = GT[u].astype(f32)
        sqa[...] += jnp.sum((v * v).reshape(SUB, DEV, LANES), axis=0)
        @pl.when(u % MATS > 0)
        def _(): cpy(GT.at[u], gt_o.at[u], gtsem).start()
        @pl.when(u % MATS == 0)
        def _():
            each(0, DEV, lambda i: a2a(u, i))
    LAST = TWO * len((S1, S2, S3, S4, S5))
    STAGES = ((S5, LAST), (S4, LAST - TWO), (S3, LAST - RING), (S2, RING), (S2x, NT), (S1, TWO))
    def slot(t):
        for S, lag in STAGES:
            @pl.when(jnp.logical_and(t >= lag, t < NU + lag))
            def _(): S(t - lag)

    each(0, MATS, A0)
    for l in range(TWO):
        wt(staged[l], ownsem.at[l])
        cpy(staged[l], WD.at[l, blk(me, SH), :], ownsem.at[l]).start()
    wt(ap, psem)
    def xnorm(i):
        wide = ya[1, blk(i, CH), :].astype(f32)
        ya[1, blk(i, CH), :] = (wide * rms(wide)).astype(bf)
    each(0, T // CH, xnorm)
    cpy(ap, a0p_h, asem).start()
    def head(i):
        guard(A2, i - 1)
        @pl.when(i == 0)
        def _(): A1(i)
        A1(i + 1)
        A0(i + MATS)
    each(0, TWO, head)
    each(0, 1, A3)
    gu_load(0, 0, 0)
    each(MATS, RING, A1)
    each(NT, DEEP, A0)
    def stv(i): return acc.at[blk(i, TF2), :]
    def step1(j):
        b = par(j)
        gu_wait(b)
        hs = j % MATS
        hr = blk(hs, TF)
        @pl.when(j >= MATS)
        def _(): wt(H.at[cut(TF)], hsem.at[hs])
        @pl.when(j > 0)
        def _(): guard(A2, j + 1)
        def sub(s):
            @pl.when(j > 0)
            def _(): wt(stv(0), stsem.at[s])
            for q in range(NCH):
                t, cols = pl.ds(pl.multiple_of(s * TB + q * TC, TC), TC), pl.ds(q * TC, TC)
                gu = dot_(wgu[b], ya[1, t, :], 0, 1)
                g, u = gu[:TF], gu[TF:]
                sg = jax.nn.sigmoid(g)
                si = g * sg
                acc[pl.ds(mul(s, TF2), TF), cols] = si
                acc[pl.ds(pl.multiple_of(s * TF2 + TF, TF), TF), cols] = u * (sg + si * (1 - sg))
                H[hr, t] = (si * u).astype(bf)
            cpy(stv(s), AB_h.at[TWO * j + s], stsem.at[s]).start()
            @pl.when(s == 0)
            def _():
                @pl.when(j == 0)
                def _(): A2(j + 1)
                guard(A3, j + 1)
                @pl.when(j < NT - 1)
                def _(): gu_load(0, j + 1, 1 - b)
                @pl.when(j == NT - 1)
                def _(): cpy(WD.at[0, pl.ds(TF3, TF2), :], wdb, wdsem.at[TWO]).start()
                guard(A1, j + RING)
                guard(A0, j + DEEP)
        each(0, TWO, sub)
        cpy(H.at[hr], h_h.at[blk(j, TF), :], hsem.at[hs]).start()
    each(0, NT, step1)
    for i in range(TWO): wt(stv(0), stsem.at[i])
    wt(ap, asem)
    start(permuted(x_h, ap, psem))
    lo, mid = cut(TF2), wgu.at[0, cut(TF), cut(D)]
    cpy(WD.at[0, pl.ds(TF2, TF), :], mid, wdsem.at[0]).start()
    acc[0:T, :] = jnp.zeros((T, D), f32)
    def down(i):
        @pl.when(i == 1)
        def _(): wt(H.at[lo], hsem.at[MATS])
        wt(wdb, wdsem.at[TWO])
        def halves(h): acc[blk(h, TB), :] += dot_(H[lo, blk(h, TB)], wdb[...], 0, 0)
        each(0, TWO, halves)
        @pl.when(i == 0)
        def _():
            for k in range(TWO): wt(H.at[cut(TF)], hsem.at[k])
            cpy(h_h.at[lo], H.at[lo], hsem.at[MATS]).start()
            cpy(WD.at[0, lo, :], wdb, wdsem.at[TWO]).start()
            A2(i + DEEP)
            A1(i + NA - MATS)
            A0(i + NA - 1)
            wt(mid, wdsem.at[0])
            def halves(h): acc[blk(h, TB), :] += dot_(H[TF2:TF3, blk(h, TB)], wgu[0, 0:TF, 0:D], 0, 0)
            each(0, TWO, halves)
        A3(i + DEEP)
        A2(i + DEEP + 1)
        @pl.when(i == 0)
        def _(): A1(i + NA - TWO)
    each(0, TWO, down)
    gu_load(1, 0, 1)
    d_load(1, 0, 0)
    wt(H.at[cut(TF)], hsem.at[TWO])
    wt(ap, psem)
    def h1s(b): return G.at[b, cut(CH)]
    def fin(i):
        b, r = par(i), blk(i, CH)
        @pl.when(i >= TWO)
        def _(): wt(h1s(0), hsem.at[b])
        h1 = (ya[1, r, :].astype(f32) + acc[r, :].astype(bf).astype(f32)).astype(bf)
        G[b, 0:CH] = h1
        cpy(h1s(b), h1p_h.at[r], hsem.at[b]).start()
        wide = h1.astype(f32)
        ya[1, r, :] = (wide * rms(wide)).astype(bf)
        acc[r, :] = jnp.zeros((CH, D), f32)
    each(0, T // CH, fin)
    for b in range(TWO): wt(h1s(0), hsem.at[b])
    def after(i):
        A3(i)
        A1(i + MATS)
    each(DEEP + TWO, DEEP + MATS, after)
    wt(dyp, dysem)

    def h1l(k): return cpy(h1p_h.at[pl.ds(k * D, D)], H.at[cut(D), pl.ds(k * D, D)], hsem.at[k])
    def abl(j, s): return cpy(AB_h.at[TWO * j + s], stv(s), stsem.at[s])
    def hload(j): return cpy(h_h.at[blk(j, TF), :], H.at[cut(TF)], hsem.at[TWO])
    def layer1(k, b):
        gu_wait(b)
        @pl.when(k + 1 < NT)
        def _(): gu_load(1, k + 1, 1 - b)
        def half(h):
            for q in range(NCH):
                t = pl.ds(pl.multiple_of(h * TB + q * TC, TC), TC)
                gu = dot_(wgu[b], ya[1, t, :], 0, 1)
                g, u = gu[:TF], gu[TF:]
                dh = dot_(wdb[blk(par(k), TF)], ya[0, t, :], 1, 1).astype(bf).astype(f32)
                sg = jax.nn.sigmoid(g)
                si = g * sg
                H[0:TF, t] = (si * u).astype(bf)
                H[TF2:TF3, t] = (dh * si).astype(bf)
                H[TF:TF2, t] = (dh * u * (sg + si * (1 - sg))).astype(bf)
            @pl.when(h == 0)
            def _(): guard(A2, k + DEEP + MATS)
        each(0, TWO, half)
        guard(A3, k + DEEP + MATS)
    def between():
        cpy(a0p_h, ap, asem).start()
        for k in range(TWO): wt(H.at[cut(D), cut(D)], hsem.at[k])
        def nb(i):
            r = blk(i, CH)
            wide = H[blk(ring(i), CH), blk(i // RING, D)].astype(f32)
            scale = rms(wide)
            da = acc[r, :].astype(bf).astype(f32)
            inner = jnp.mean(da * wide, -1, keepdims=True)
            dw = (da * scale - wide * (scale * scale * scale * inner)).astype(bf)
            ya[0, r, :] = (ya[0, r, :].astype(f32) + dw.astype(f32)).astype(bf)
            @pl.when(i == TF2 // CH - 1)
            def _(): abl(0, 0).start()
        each(0, T // CH, nb)
        abl(0, 1).start()
        hload(0).start()
        wt(ap, asem)
    def layer0(j, b):
        def sub(s):
            abl(j, s).wait()
            for q in range(NCH):
                t, cols = pl.ds(pl.multiple_of(s * TB + q * TC, TC), TC), pl.ds(q * TC, TC)
                dh = dot_(wdb[blk(b, TF)], ya[0, t, :], 1, 1).astype(bf).astype(f32)
                H[TF2:TF3, t] = (dh * acc[pl.ds(mul(s, TF2), TF), cols]).astype(bf)
                H[TF:TF2, t] = (dh * acc[pl.ds(pl.multiple_of(s * TF2 + TF, TF), TF), cols]).astype(bf)
            @pl.when(j + 1 < NT)
            def _(): abl(j + 1, s).start()
        each(0, TWO, sub)
        hload(j).wait()
    def tile(k):
        b, gb = par(k), par(k + 1)
        d_wait(b)
        @pl.when(k + 1 < NT)
        def _(): d_load(1, k + 1, 1 - b)
        @pl.when(jnp.logical_and(k + 1 >= NT, k + 1 < TWO * NT))
        def _(): d_load(0, k + 1 - NT, 1 - b)
        @pl.when(k < NT)
        def _(): layer1(k, gb)
        @pl.when(k == NT)
        def _(): between()
        @pl.when(k >= NT)
        def _(): layer0(k - NT, b)
        def mat(m):
            t = MATS * k + m
            slot(t)
            G[par(t)] = dot_(H[blk(m, TF)], ya[(m + 1) // TWO], 1, 0).astype(bf)
            S0(t)
            @pl.when(jnp.logical_and(k < NT, m < TWO))
            def _(): acc[blk(m, TB), :] += dot_(H[TF:TF3, blk(m, TB)], wgu[gb], 0, 1)
            @pl.when(jnp.logical_and(k == NT - 1, m == 1))
            def _():
                for q in range(TWO): h1l(q).start()
            @pl.when(jnp.logical_and(jnp.logical_and(k >= NT, k + 1 < TWO * NT), m == 0))
            def _(): hload(k - NT + 1).start()
        each(0, MATS, mat)
    each(0, TWO * NT, tile)
    each(NU, NU + LAST, slot)

    SQ[me] = sqa[...]
    def sqc(e, i): return rd(sqa, SQ.at[i], sqs, sqr, (0, r_, (me + e) % DEV))
    for e in range(1, DEV): sqc(e, me).start()
    def drain(n, k, sem): wt(GT.at[cut(n), cut(k)], sem)
    drain(NU - TWO * NT, TF, gtsem)
    drain(TWO, SH, locsem)
    drain(TWO * (DEV - 1), SH, a2s)
    for l in range(TWO): drain(DEV - 1, SH, a2r.at[l])
    for sem in (sqs, sqr): wt(SQ.at[cut(DEV - 1)], sem)
    tot = SQ[0]
    for i in range(1, DEV): tot = tot + SQ[i]
    sq_o[...] = tot


def train(x, dy, wg, wu, wd):
    hbm = pl.BlockSpec(memory_space=pl.ANY)
    V, S = pltpu.VMEM, pltpu.SemaphoreType.DMA
    b = (SUB, LANES)
    r3 = (RING, TWO, MATS)
    one, two, three, four, six = S, S((TWO,)), S((MATS,)), S((RING,)), S((DEEP,))
    outs = [sds((NU, TF, LANES), bf), sds((TWO, SH, D), bf), sds((DEV, LANES), f32), sds((TWO, DEV, TWO, LANES, F), bf), sds((TWO, F, D), bf),
            sds((T, D), bf), sds((T, D), bf), sds((NT * TWO, TF2, D), f32), sds((F, T), bf)]
    specs = [hbm] * len(outs)
    specs[TWO] = pl.BlockSpec(memory_space=pltpu.VMEM)
    return pl.pallas_call(
        step_kernel,
        out_shape=outs, in_specs=[hbm] * (MATS + TWO), out_specs=specs,
        scratch_shapes=[
            V((TWO, T, D), bf), V((TWO * TF2, D), f32), V((TWO, D, TF2), bf), V((TF2, D), bf), V((TF3, T), bf), V((TWO, TF, D), bf), V((RING, TF, HALF), bf),
            V((MATS, TWO, RING, RING) + b, bf), V(r3 + (RING,) + b, bf), V((TWO, RING, TWO) + b, bf), V((DEEP, MATS, TWO) + b, bf), V((TWO, TWO) + b, bf), V((RING, TWO, RING) + b, bf),
            V((NU, TF, LANES), bf), V((DEV, LANES), f32), V((DEV, DEV, LANES), f32),
            one, one, one, two, two, three, two, S((RING,)), one, one,
            two, four, four, four, two, six, two, four, two, four, one, two,
            six, six, S((NA,)), S((NA,)), six, six, six, S((NA,)), one, one],
        compiler_params=pltpu.CompilerParams(collective_id=0, has_side_effects=True, vmem_limit_bytes=VMEM_LIMIT),
        name="train")(x, dy, wg, wu, wd)


def optimizer(sq, GT, GD, w, m, v):
    def kernel(sq, gg, gu, gd, *r):
        tot = jnp.sum(jnp.sum(sq[...], axis=0, keepdims=True), axis=1, keepdims=True)
        factor = jnp.minimum(1.0, 0.5 * lax.rsqrt(tot / (TWO * MATS * D * F) + 1e-30))
        ws, ms, vs, wo, mo, vo = (r[i * MATS:(i + 1) * MATS] for i in range(TWO * MATS))
        for i, block in enumerate((gg, gu, gd)):
            g = block[0].astype(f32)
            g = (g if i == TWO else g.T) * factor
            mm = 0.9 * ms[i][0] + 0.1 * g
            vv = 0.95 * vs[i][0] + 0.05 * g * g
            ww = ws[i][0].astype(f32)
            wo[i][0] = (ww - 0.02 * (mm * lax.rsqrt(vv + 1e-8) + 0.1 * ww)).astype(bf)
            mo[i][0], vo[i][0] = mm, vv
    def tile(i): return pl.BlockSpec((1, TF, LANES), lambda l, j: ((1 - l) * OFFLAY + MATS * j + i, 0, 0))
    a, d = pl.BlockSpec((1, LANES, TF), lambda l, j: (l, 0, j)), pl.BlockSpec((1, SUB, D), lambda l, j: (l, j, 0))
    outs = tuple(sds(q.shape, t) for t in (bf, f32, f32) for q in w)
    return pl.pallas_call(
        kernel, grid=(TWO, NT), in_specs=[pl.BlockSpec((DEV, LANES), lambda l, j: (0, 0)), tile(1), tile(TWO), d] + [a, a, d] * MATS,
        out_specs=(a, a, d) * MATS, out_shape=outs,
        compiler_params=pltpu.CompilerParams(vmem_limit_bytes=VMEM_LIMIT, dimension_semantics=("arbitrary",) * TWO),
        name="optimizer")(sq, GT, GT, GD, *w, *m, *v)


def solution(mesh):
    def step(x, dy, *arrays):
        w, m, v = (arrays[i:i + MATS] for i in range(0, len(arrays), MATS))
        GT, GD, sq = train(x[0], dy[0], *w)[:MATS]
        return optimizer(sq, GT, GD, w, m, v)
    states, cuts = P(("rep", "r", "s"), None, None), P(None, "s", None)
    return jax.shard_map(step, mesh=mesh, in_specs=(states, states) + (cuts,) * (MATS * MATS), out_specs=(P("rep", "s", None),) * (MATS * MATS), check_vma=False)
```

```python
import jax, jax.numpy as jnp
from jax import lax
from jax.experimental import pallas as pl
from jax.experimental.pallas import tpu as pltpu
from jax.sharding import PartitionSpec as P

bf, f32 = jnp.bfloat16, jnp.float32
T, D, F, TF = 2048, 1024, 3200, 640
TWO, MATS, RING = 2, 3, 4
NT = F // TF
NU = TWO * MATS * NT
NA = TWO * NT + TWO
DEEP = 6
LANES, SUB, HALF, CH, SH = 128, 80, 512, 256, 400
NCH = 2
DEV = D // LANES
TF2, TF3, TB = TWO * TF, MATS * TF, T // TWO
TC = TB // NCH
AROWS = LANES // DEV
OFFS = range(1, RING)
VMEM_LIMIT = 67043328
EPS = 1e-6
OFFLAY = NU // TWO


def sds(s, d): return jax.ShapeDtypeStruct(s, d)
def dot_(a, b, ca, cb): return lax.dot_general(a, b, (((ca,), (cb,)), ((), ())), preferred_element_type=f32)
def mul(i, n): return pl.multiple_of(i * n, n)
def blk(i, n): return pl.ds(mul(i, n), n)
def cut(n): return pl.ds(0, n)
def cpy(src, dst, sem): return pltpu.make_async_copy(src, dst, sem)
def wt(ref, sem): cpy(ref, ref, sem).wait()
def start(cs):
    for q in cs: q.start()
def each(lo, hi, f):
    def g(i, _):
        f(i)
        return _
    lax.fori_loop(lo, hi, g, 0)
def rms(wide): return lax.rsqrt(jnp.mean(wide * wide, -1, keepdims=True) + EPS)
def pc(k): return (k % TWO) * RING + k // TWO
def par(u): return u % TWO
def ring(u): return u % RING


def step_kernel(x_h, dy_h, wg_i, wu_i, wd_i,
                gt_o, gd_o, sq_o, WGU, WD, a0p_h, h1p_h, AB_h, h_h,
                ya, acc, wgu, wdb, H, G, R0, Pb, R1, Q, R2, U, R3, GT, sqa, SQ,
                dysem, asem, psem, ownsem, gusem, wdsem, stsem, hsem, gtsem, locsem,
                s0s, s0r, s1s, s1r, s2s, s2r, s3s, s3r, s4s, s4r, a2s, a2r,
                ag0s, ag0r, agds, agdr, ag1s, ag1r, ag2s, ag2r, sqs, sqr):
    r_, me = lax.axis_index("r"), lax.axis_index("s")
    x, y, z, c = me // TWO, r_ // RING, r_ % RING, me % TWO
    own = c * RING + x
    def dev(x, y, z, c): return (0, y * RING + z, x * TWO + c)
    def xdev(d): return dev(ring(x + d), y, z, c)
    def ydev(d): return dev(x, ring(y + d), z, c)
    def zdev(d): return dev(x, y, ring(z + d), c)
    part = dev(x, y, z, 1 - c)
    AX = ((0, y, ydev), (1, z, zdev))
    dyp, ap = ya.at[0], ya.at[1]
    bar = pltpu.get_barrier_semaphore()
    peers = [part] + [f(d) for f in (xdev, ydev, zdev) for d in OFFS] + [dev(ring(x + d), y, z, 1 - c) for d in OFFS]
    for p in peers: pl.semaphore_signal(bar, inc=1, device_id=p, device_id_type=pl.DeviceIdType.MESH)
    def rd(src, dst, ss, rs, d):
        return pltpu.make_async_remote_copy(src_ref=src, dst_ref=dst, send_sem=ss, recv_sem=rs, device_id=d, device_id_type=pl.DeviceIdType.MESH)
    def same(ref, ss, rs, d): return rd(ref, ref, ss, rs, d)
    def permuted(src, dst, sem): return [cpy(src.at[:, pl.ds(k * LANES, LANES)], dst.at[:, pl.ds(pc(k) * LANES, LANES)], sem) for k in range(DEV)]
    start(permuted(x_h, ap, psem))
    staged = [wdb.at[pl.ds(l * TF, SH)] for l in range(TWO)]
    for l in range(TWO): start(permuted(wd_i.at[l], staged[l], ownsem.at[l]))
    start(permuted(dy_h, dyp, dysem))
    sqa[...] = jnp.zeros_like(sqa)
    pl.semaphore_wait(bar, len(peers))

    def gu_load(l, j, b):
        for m, inp in enumerate((wg_i, wu_i)):
            cols = pl.ds(m * TF, TF)
            cpy(inp.at[l, :, blk(j, TF)], wgu.at[b, blk(own, LANES), cols], gusem.at[b]).start()
            def one(e):
                k = (own + e) % DEV
                cpy(WGU.at[l, k, m, :, blk(j, TF)], wgu.at[b, blk(k, LANES), cols], gusem.at[b]).start()
            each(1, DEV, one)
    def gu_wait(b): wt(wgu.at[b], gusem.at[b])
    def d_load(l, j, b): cpy(WD.at[l, blk(j, TF), :], wdb.at[blk(b, TF)], wdsem.at[b]).start()
    def d_wait(b): wt(wdb.at[blk(b, TF)], wdsem.at[b])

    def q16(h, q): return pl.ds(pl.multiple_of(h * (LANES // TWO) + q * AROWS, AROWS), AROWS)
    def colq(h, q): return blk(pc(RING * h + q), LANES)
    def fork(u, fg, fd):
        @pl.when(u % (NT + TWO) < NT)
        def _(): fg(u // (NT + TWO), u % (NT + TWO))
        @pl.when(u % (NT + TWO) >= NT)
        def _(): fd(u - NT)
    def both(ref, ss, rs, b):
        wt(ref, ss.at[b])
        wt(ref, rs.at[b])
    def A0(u):
        b = u % DEEP
        def fg(l, j):
            for m, inp in enumerate((wg_i, wu_i)):
                def one(i):
                    for h, q, _ in AX: rd(inp.at[l, q16(h, q), blk(j, TF)], WGU.at[l, own, m, q16(h, q), blk(j, TF)], ag0s.at[b], ag0r.at[b], xdev(i + 1)).start()
                each(0, MATS, one)
                rd(inp.at[l, :, blk(j, TF)], WGU.at[l, own, m, :, blk(j, TF)], agds.at[u], agdr.at[u], part).start()
        def fd(l):
            wt(WD.at[0, cut(SH), :], ownsem.at[l])
            def one(i):
                for h, q, _ in AX: same(WD.at[l, blk(me, SH), colq(h, q)], ag0s.at[b], ag0r.at[b], xdev(i + 1)).start()
            each(0, MATS, one)
            same(WD.at[l, blk(me, SH), :], agds.at[u], agdr.at[u], part).start()
        fork(u, fg, fd)
    def A1(u):
        b = u % DEEP
        def fg(l, j):
            both(WGU.at[0, cut(DEEP), :, cut(AROWS), cut(TF)], ag0s, ag0r, b)
            def one(i):
                k, d = c * RING + ring(x + i // MATS + 1), i % MATS
                for h, q, f in AX: same(WGU.at[l, k, :, q16(h, q), blk(j, TF)], ag1s.at[b], ag1r.at[b], f(d + 1)).start()
            each(0, MATS * MATS, one)
        def fd(l):
            both(WD.at[0, cut(DEEP * SH), cut(LANES)], ag0s, ag0r, b)
            def one(i):
                k, d = TWO * ring(x + i // MATS + 1) + c, i % MATS
                for h, q, f in AX: same(WD.at[l, blk(k, SH), colq(h, q)], ag1s.at[b], ag1r.at[b], f(d + 1)).start()
            each(0, MATS * MATS, one)
        fork(u, fg, fd)
    gu1, gu3 = WGU.at[0, 0, :, :, cut(TF)], WGU.at[0, cut(MATS), :, :, cut(TF)]
    wd1, wd3 = WD.at[0, cut(SH), :], WD.at[0, cut(MATS * SH), :]
    def A2(u):
        b = u % DEEP
        def fg(l, j):
            both(WGU.at[0, cut(DEEP), :, cut(MATS * AROWS), cut(TF)], ag1s, ag1r, b)
            each(1, RING, lambda i: same(WGU.at[l, c * RING + ring(x + i), :, :, blk(j, TF)], ag2s.at[b], ag2r.at[u], part).start())
        def fd(l):
            both(WD.at[0, cut(DEEP * SH), cut(MATS * LANES)], ag1s, ag1r, b)
            each(1, RING, lambda i: same(WD.at[l, blk(TWO * ring(x + i) + c, SH), :], ag2s.at[b], ag2r.at[u], part).start())
        fork(u, fg, fd)
    def A3(u):
        b = u % DEEP
        def done(one, three):
            for ref, sem in ((one, agds.at[u]), (one, agdr.at[u]), (three, ag2s.at[b]), (three, ag2r.at[u])): wt(ref, sem)
        fork(u, lambda l, j: done(gu1, gu3), lambda l: done(wd1, wd3))
    def guard(A, u):
        @pl.when(jnp.logical_and(u >= 0, u < NA))
        def _(): A(u)

    def c0(u): return rd(G.at[par(u), :, blk(1 - c, HALF)], R0.at[ring(u)], s0s.at[par(u)], s0r.at[ring(u)], part)
    def mat_(u): return u % MATS
    def deep(u): return u % DEEP
    def c1(u):
        return [rd(Pb.at[mat_(u), h, ring(q + d)], R1.at[ring(u), h, d - 1], s1s.at[ring(u)], s1r.at[ring(u)], f(d)) for d in OFFS for h, q, f in AX]
    def c1x(u): return [rd(Pb.at[mat_(u), :, :, ring(x + d)], R1.at[ring(u), :, d - 1], s1s.at[ring(u)], s1r.at[ring(u)], xdev(d)) for d in OFFS]
    def c2(u): return [rd(Q.at[ring(u), ring(x + d)], R2.at[deep(u), d - 1], s2s.at[ring(u)], s2r.at[deep(u)], xdev(d)) for d in OFFS]
    def c2x(u):
        return [rd(Q.at[ring(u), ring(q + d), h], R2.at[deep(u), d - 1, h], s2s.at[ring(u)], s2r.at[deep(u)], f(d)) for d in OFFS for h, q, f in AX]
    def either(u, f, *args):
        @pl.when(mat_(u) > 0)
        def _(): f(*args[0])
        @pl.when(mat_(u) == 0)
        def _(): f(*args[1])
    def c3(u):
        return [rd(U.at[ring(u), h], R3.at[deep(u), h, q], s3s.at[ring(u)], s3r.at[deep(u)], f(d)) for d in OFFS for h, q, f in ((0, z, zdev), (1, y, ydev))]
    def rows(h, q): return pl.ds(pl.multiple_of(h * (TF // TWO) + q * SUB, SUB), SUB)
    def c4(u):
        return [same(GT.at[u, rows(h, q)], s4s.at[ring(u)], s4r.at[deep(u)], f(d)) for d in OFFS for h, q, f in AX]
    def S0(u): c0(u).start()
    def S1(u):
        c0(u).wait()
        for i in range(DEV):
            for k in range(RING):
                mine = G[par(u), pl.ds(i * SUB, SUB), blk(c * RING + k, LANES)]
                Pb[mat_(u), i // RING, i % RING, k] = (mine.astype(f32) + R0[ring(u), pl.ds(i * SUB, SUB), pl.ds(k * LANES, LANES)].astype(f32)).astype(bf)
        either(u, lambda way: start(way(u)), (c1,), (c1x,))
    def added(first, rest):
        s = first.astype(f32)
        for q in rest: s = s + q.astype(f32)
        return s.astype(bf)
    def second(u, first, send):
        wt(R1.at[0], s1s.at[ring(u)])
        wt(R1.at[0], s1r.at[ring(u)])
        for h, mine, _ in AX:
            for k in range(RING): Q[ring(u), k, h] = added(first(h, mine, k), [R1[ring(u), h, d, k] for d in range(MATS)])
        start(send(u))
    def S2(u):
        @pl.when(mat_(u) > 0)
        def _(): second(u, lambda h, mine, k: Pb[mat_(u), h, mine, k], c2)
    def S2x(u):
        @pl.when(mat_(u) == 0)
        def _(): second(u, lambda h, mine, k: Pb[mat_(u), h, k, x], c2x)
    def S3(u):
        wt(R2.at[0], s2s.at[ring(u)])
        wt(R2.at[0], s2r.at[deep(u)])
        def go(*mine):
            for h in range(TWO): U[ring(u), h] = added(Q[ring(u), mine[h], h], [R2[deep(u), d, h] for d in range(MATS)])
        either(u, go, (x, x), (y, z))
        start(c3(u))
    def S4(u):
        wt(R2.at[0], s3s.at[ring(u)])
        wt(R2.at[0], s3r.at[deep(u)])
        R3[deep(u), 0, z] = U[ring(u), 0]
        R3[deep(u), 1, y] = U[ring(u), 1]
        for h, q, _ in AX:
            s = R3[deep(u), h, 0].astype(f32)
            for d in OFFS: s = s + R3[deep(u), h, d].astype(f32)
            GT[u, rows(h, q)] = s.astype(bf)
        start(c4(u))
    def a2a(u, i):
        lay, n = u // OFFLAY, DEV * ((u % OFFLAY) // MATS) + i
        to = n // NT
        src, dst = GT.at[u, blk(i, SUB)], gd_o.at[1 - lay, blk(n - NT * to, SUB), blk(me, LANES)]
        @pl.when(to != me)
        def _(): rd(src, dst, a2s, a2r.at[lay], (0, r_, to)).start()
        @pl.when(to == me)
        def _(): cpy(src, dst, locsem).start()
    def S5(u):
        wt(R2.at[0], s4s.at[ring(u)])
        wt(R2.at[0], s4r.at[deep(u)])
        v = GT[u].astype(f32)
        sqa[...] += jnp.sum((v * v).reshape(SUB, DEV, LANES), axis=0)
        @pl.when(u % MATS > 0)
        def _(): cpy(GT.at[u], gt_o.at[u], gtsem).start()
        @pl.when(u % MATS == 0)
        def _():
            each(0, DEV, lambda i: a2a(u, i))
    LAST = TWO * len((S1, S2, S3, S4, S5))
    STAGES = ((S2, RING, NU), (S2x, NT, NU), (S3, LAST - RING, NU), (S1, TWO, NU - 1), (S4, LAST - TWO, NU), (S5, LAST, NU))
    def slot(t):
        for S, lag, end in STAGES:
            @pl.when(jnp.logical_and(t >= lag, t < end + lag))
            def _(): S(t - lag)
            if S is S1:
                @pl.when(t == NU)
                def _(): S1(t - 1)

    each(0, MATS, A0)
    for l in range(TWO):
        wt(staged[l], ownsem.at[l])
        cpy(staged[l], WD.at[l, blk(me, SH), :], ownsem.at[l]).start()
    wt(ap, psem)
    def xnorm(i):
        wide = ya[1, blk(i, CH), :].astype(f32)
        ya[1, blk(i, CH), :] = (wide * rms(wide)).astype(bf)
    each(0, T // CH, xnorm)
    cpy(ap, a0p_h, asem).start()
    def head(i):
        guard(A2, i - 1)
        @pl.when(i == 0)
        def _(): A1(i)
        A1(i + 1)
        A0(i + MATS)
    each(0, TWO, head)
    each(0, 1, A3)
    gu_load(0, 0, 0)
    each(MATS, RING, A1)
    each(NT, DEEP, A0)
    def stv(i): return acc.at[blk(i, TF2), :]
    def step1(j):
        b = par(j)
        gu_wait(b)
        hs = j % MATS
        hr = blk(hs, TF)
        @pl.when(j >= MATS)
        def _(): wt(H.at[cut(TF)], hsem.at[hs])
        @pl.when(j > 0)
        def _(): guard(A2, j + 1)
        def sub(s):
            @pl.when(j > 0)
            def _(): wt(stv(0), stsem.at[s])
            for q in range(NCH):
                t, cols = pl.ds(pl.multiple_of(s * TB + q * TC, TC), TC), pl.ds(q * TC, TC)
                gu = dot_(wgu[b], ya[1, t, :], 0, 1)
                g, u = gu[:TF], gu[TF:]
                sg = jax.nn.sigmoid(g)
                si = g * sg
                acc[pl.ds(mul(s, TF2), TF), cols] = si
                acc[pl.ds(pl.multiple_of(s * TF2 + TF, TF), TF), cols] = u * (sg + si * (1 - sg))
                H[hr, t] = (si * u).astype(bf)
            cpy(stv(s), AB_h.at[TWO * j + s], stsem.at[s]).start()
            @pl.when(s == 0)
            def _():
                @pl.when(j == 0)
                def _(): A2(j + 1)
                guard(A3, j + 1)
                @pl.when(j < NT - 1)
                def _(): gu_load(0, j + 1, 1 - b)
                @pl.when(j == NT - 1)
                def _(): cpy(WD.at[0, pl.ds(TF3, TF2), :], wdb, wdsem.at[TWO]).start()
                guard(A1, j + RING)
                guard(A0, j + DEEP)
        each(0, TWO, sub)
        cpy(H.at[hr], h_h.at[blk(j, TF), :], hsem.at[hs]).start()
    each(0, NT, step1)
    for i in range(TWO): wt(stv(0), stsem.at[i])
    wt(ap, asem)
    start(permuted(x_h, ap, psem))
    lo, mid = cut(TF2), wgu.at[0, cut(TF), cut(D)]
    cpy(WD.at[0, pl.ds(TF2, TF), :], mid, wdsem.at[0]).start()
    def down(i):
        @pl.when(i == 1)
        def _(): wt(H.at[lo], hsem.at[MATS])
        wt(wdb, wdsem.at[TWO])
        def halves(h):
            term = lambda: dot_(H[lo, blk(h, TB)], wdb[...], 0, 0)
            @pl.when(i == 0)
            def _(): acc[blk(h, TB), :] = term()
            @pl.when(i > 0)
            def _(): acc[blk(h, TB), :] += term()
        each(0, TWO, halves)
        @pl.when(i == 0)
        def _():
            for k in range(TWO): wt(H.at[cut(TF)], hsem.at[k])
            cpy(h_h.at[lo], H.at[lo], hsem.at[MATS]).start()
            cpy(WD.at[0, lo, :], wdb, wdsem.at[TWO]).start()
            A2(i + DEEP)
            A1(i + NA - MATS)
            A0(i + NA - 1)
            wt(mid, wdsem.at[0])
            def halves(h): acc[blk(h, TB), :] += dot_(H[TF2:TF3, blk(h, TB)], wgu[0, 0:TF, 0:D], 0, 0)
            each(0, TWO, halves)
        A3(i + DEEP)
        A2(i + DEEP + 1)
        @pl.when(i == 0)
        def _(): A1(i + NA - TWO)
    each(0, TWO, down)
    gu_load(1, 0, 1)
    d_load(1, 0, 0)
    wt(H.at[cut(TF)], hsem.at[TWO])
    wt(ap, psem)
    def h1s(b): return G.at[b, cut(CH)]
    def fin(i):
        b, r = par(i), blk(i, CH)
        @pl.when(i >= TWO)
        def _(): wt(h1s(0), hsem.at[b])
        h1 = (ya[1, r, :].astype(f32) + acc[r, :].astype(bf).astype(f32)).astype(bf)
        G[b, 0:CH] = h1
        cpy(h1s(b), h1p_h.at[r], hsem.at[b]).start()
        wide = h1.astype(f32)
        ya[1, r, :] = (wide * rms(wide)).astype(bf)
        acc[r, :] = jnp.zeros((CH, D), f32)
    each(0, T // CH, fin)
    for b in range(TWO): wt(h1s(0), hsem.at[b])
    def after(i):
        A3(i)
        A1(i + MATS)
    each(DEEP + TWO, DEEP + MATS, after)
    wt(dyp, dysem)

    def h1l(k): return cpy(h1p_h.at[pl.ds(k * D, D)], H.at[cut(D), pl.ds(k * D, D)], hsem.at[k])
    def abl(j, s): return cpy(AB_h.at[TWO * j + s], stv(s), stsem.at[s])
    def hload(j): return cpy(h_h.at[blk(j, TF), :], H.at[cut(TF)], hsem.at[TWO])
    def layer1(k, b):
        gu_wait(b)
        @pl.when(k + 1 < NT)
        def _(): gu_load(1, k + 1, 1 - b)
        def half(h):
            for q in range(NCH):
                t = pl.ds(pl.multiple_of(h * TB + q * TC, TC), TC)
                gu = dot_(wgu[b], ya[1, t, :], 0, 1)
                g, u = gu[:TF], gu[TF:]
                dh = dot_(wdb[blk(par(k), TF)], ya[0, t, :], 1, 1).astype(bf).astype(f32)
                sg = jax.nn.sigmoid(g)
                si = g * sg
                H[0:TF, t] = (si * u).astype(bf)
                H[TF2:TF3, t] = (dh * si).astype(bf)
                H[TF:TF2, t] = (dh * u * (sg + si * (1 - sg))).astype(bf)
            @pl.when(h == 0)
            def _(): guard(A2, k + DEEP + MATS)
        each(0, TWO, half)
        guard(A3, k + DEEP + MATS)
    def between():
        cpy(a0p_h, ap, asem).start()
        for k in range(TWO): wt(H.at[cut(D), cut(D)], hsem.at[k])
        def nb(i):
            r = blk(i, CH)
            wide = H[blk(ring(i), CH), blk(i // RING, D)].astype(f32)
            scale = rms(wide)
            da = acc[r, :].astype(bf).astype(f32)
            inner = jnp.mean(da * wide, -1, keepdims=True)
            dw = (da * scale - wide * (scale * scale * scale * inner)).astype(bf)
            ya[0, r, :] = (ya[0, r, :].astype(f32) + dw.astype(f32)).astype(bf)
            @pl.when(i == TF2 // CH - 1)
            def _(): abl(0, 0).start()
        each(0, T // CH, nb)
        abl(0, 1).start()
        hload(0).start()
        wt(ap, asem)
    def layer0(j, b):
        def sub(s):
            abl(j, s).wait()
            for q in range(NCH):
                t, cols = pl.ds(pl.multiple_of(s * TB + q * TC, TC), TC), pl.ds(q * TC, TC)
                dh = dot_(wdb[blk(b, TF)], ya[0, t, :], 1, 1).astype(bf).astype(f32)
                H[TF2:TF3, t] = (dh * acc[pl.ds(mul(s, TF2), TF), cols]).astype(bf)
                H[TF:TF2, t] = (dh * acc[pl.ds(pl.multiple_of(s * TF2 + TF, TF), TF), cols]).astype(bf)
            @pl.when(j + 1 < NT)
            def _(): abl(j + 1, s).start()
        each(0, TWO, sub)
        hload(j).wait()
    def tile(k):
        b, gb = par(k), par(k + 1)
        d_wait(b)
        @pl.when(k + 1 < NT)
        def _(): d_load(1, k + 1, 1 - b)
        @pl.when(jnp.logical_and(k + 1 >= NT, k + 1 < TWO * NT))
        def _(): d_load(0, k + 1 - NT, 1 - b)
        @pl.when(k < NT)
        def _(): layer1(k, gb)
        @pl.when(k == NT)
        def _(): between()
        @pl.when(k >= NT)
        def _(): layer0(k - NT, b)
        def mat(m):
            t = MATS * k + m
            slot(t)
            G[par(t)] = dot_(H[blk(m, TF)], ya[(m + 1) // TWO], 1, 0).astype(bf)
            S0(t)
            @pl.when(jnp.logical_and(k < NT, m < TWO))
            def _(): acc[blk(m, TB), :] += dot_(H[TF:TF3, blk(m, TB)], wgu[gb], 0, 1)
            @pl.when(jnp.logical_and(k == NT - 1, m == 1))
            def _():
                for q in range(TWO): h1l(q).start()
            @pl.when(jnp.logical_and(jnp.logical_and(k >= NT, k + 1 < TWO * NT), m == 0))
            def _(): hload(k - NT + 1).start()
        each(0, MATS, mat)
    each(0, TWO * NT, tile)
    each(NU, NU + LAST, slot)

    SQ[me] = sqa[...]
    def sqc(e, i): return rd(sqa, SQ.at[i], sqs, sqr, (0, r_, (me + e) % DEV))
    for e in range(1, DEV): sqc(e, me).start()
    def drain(n, k, sem): wt(GT.at[cut(n), cut(k)], sem)
    drain(NU - TWO * NT, TF, gtsem)
    drain(TWO, SH, locsem)
    drain(TWO * (DEV - 1), SH, a2s)
    for l in range(TWO): drain(DEV - 1, SH, a2r.at[l])
    for sem in (sqs, sqr): wt(SQ.at[cut(DEV - 1)], sem)
    tot = SQ[0]
    for i in range(1, DEV): tot = tot + SQ[i]
    sq_o[...] = tot


def train(x, dy, wg, wu, wd):
    hbm = pl.BlockSpec(memory_space=pl.ANY)
    V, S = pltpu.VMEM, pltpu.SemaphoreType.DMA
    b = (SUB, LANES)
    r3 = (RING, TWO, MATS)
    one, two, three, four, six = S, S((TWO,)), S((MATS,)), S((RING,)), S((DEEP,))
    outs = [sds((NU, TF, LANES), bf), sds((TWO, SH, D), bf), sds((DEV, LANES), f32), sds((TWO, DEV, TWO, LANES, F), bf), sds((TWO, F, D), bf),
            sds((T, D), bf), sds((T, D), bf), sds((NT * TWO, TF2, D), f32), sds((F, T), bf)]
    specs = [hbm] * len(outs)
    specs[TWO] = pl.BlockSpec(memory_space=pltpu.VMEM)
    return pl.pallas_call(
        step_kernel,
        out_shape=outs, in_specs=[hbm] * (MATS + TWO), out_specs=specs,
        scratch_shapes=[
            V((TWO, T, D), bf), V((TWO * TF2, D), f32), V((TWO, D, TF2), bf), V((TF2, D), bf), V((TF3, T), bf), V((TWO, TF, D), bf), V((RING, TF, HALF), bf),
            V((MATS, TWO, RING, RING) + b, bf), V(r3 + (RING,) + b, bf), V((RING, RING, TWO) + b, bf), V((DEEP, MATS, TWO) + b, bf), V((RING, TWO) + b, bf), V((DEEP, TWO, RING) + b, bf),
            V((NU, TF, LANES), bf), V((DEV, LANES), f32), V((DEV, DEV, LANES), f32),
            one, one, one, two, two, three, two, S((RING,)), one, one,
            two, four, four, four, four, six, four, six, four, six, one, two,
            six, six, S((NA,)), S((NA,)), six, six, six, S((NA,)), one, one],
        compiler_params=pltpu.CompilerParams(collective_id=0, has_side_effects=True, vmem_limit_bytes=VMEM_LIMIT),
        name="train")(x, dy, wg, wu, wd)


def optimizer(sq, GT, GD, w, m, v):
    groups = [(l, i) for l in range(TWO) for i in range(MATS)]
    def kernel(sq, GT, GD, *r):
        take = lambda k: r[k * MATS:(k + 1) * MATS]
        srcs, dsts, bufs = [take(k) for k in range(MATS)], [take(k) for k in range(MATS, DEEP)], [take(k) for k in range(DEEP, DEEP + MATS)]
        gb, gdb, isem, osem, gsem = r[MATS * (DEEP + MATS):]
        for l, i in groups:
            for k in range(MATS): cpy(srcs[k][i].at[l], bufs[k][i].at[l], isem.at[k, l, i]).start()
            if i == TWO: cpy(GD.at[l], gdb.at[l], gsem.at[l, i]).start()
            else: start([cpy(GT.at[(1 - l) * OFFLAY + MATS * j + i + 1], gb.at[l, i, j], gsem.at[l, i]) for j in range(NT)])
        tot = jnp.sum(jnp.sum(sq[...], axis=0, keepdims=True), axis=1, keepdims=True)
        factor = jnp.minimum(1.0, 0.5 * lax.rsqrt(tot / (TWO * MATS * D * F) + 1e-30))
        def out(k, l, i): return cpy(bufs[k][i].at[l], dsts[k][i].at[l], osem.at[k, l, i])
        for l, i in groups:
            for k in range(MATS): wt(bufs[k][i].at[l], isem.at[k, l, i])
            wt(gdb.at[l] if i == TWO else gb.at[l, i], gsem.at[l, i])
            wb, mb, vb = (bufs[k][i] for k in range(MATS))
            def one(j):
                at = (l, blk(j, SUB), slice(None)) if i == TWO else (l, slice(None), blk(j, TF))
                g = (gdb[at].astype(f32) if i == TWO else gb[l, i, j].astype(f32).T) * factor
                mm = 0.9 * mb[at] + 0.1 * g
                vv = 0.95 * vb[at] + 0.05 * g * g
                ww = wb[at].astype(f32)
                wb[at] = (ww - 0.02 * (mm * lax.rsqrt(vv + 1e-8) + 0.1 * ww)).astype(bf)
                mb[at], vb[at] = mm, vv
            each(0, NT, one)
            for k in range(MATS): out(k, l, i).start()
        for l, i in groups:
            for k in range(MATS): out(k, l, i).wait()
    hbm = pl.BlockSpec(memory_space=pl.ANY)
    V, S = pltpu.VMEM, pltpu.SemaphoreType.DMA
    outs = tuple(sds(q.shape, t) for t in (bf, f32, f32) for q in w)
    return pl.pallas_call(
        kernel, in_specs=[pl.BlockSpec(memory_space=pltpu.VMEM)] + [hbm] * (TWO + MATS * MATS), out_specs=(hbm,) * len(outs), out_shape=outs,
        scratch_shapes=[V(q.shape, q.dtype) for q in outs] + [V((TWO, TWO, NT, TF, LANES), bf), V((TWO, SH, D), bf), S((MATS, TWO, MATS)), S((MATS, TWO, MATS)), S((TWO, MATS))],
        compiler_params=pltpu.CompilerParams(vmem_limit_bytes=VMEM_LIMIT),
        name="optimizer")(sq, GT, GD, *w, *m, *v)


def solution(mesh):
    def step(x, dy, *arrays):
        w, m, v = (arrays[i:i + MATS] for i in range(0, len(arrays), MATS))
        GT, GD, sq = train(x[0], dy[0], *w)[:MATS]
        return optimizer(sq, GT, GD, w, m, v)
    states, cuts = P(("rep", "r", "s"), None, None), P(None, "s", None)
    return jax.shard_map(step, mesh=mesh, in_specs=(states, states) + (cuts,) * (MATS * MATS), out_specs=(P("rep", "s", None),) * (MATS * MATS), check_vma=False)
```

```python
import jax, jax.numpy as jnp
from jax import lax
from jax.experimental import pallas as pl
from jax.experimental.pallas import tpu as pltpu
from jax.sharding import PartitionSpec as P

bf, f32 = jnp.bfloat16, jnp.float32
T, D, F, TF = 2048, 1024, 3200, 640
TWO, MATS, RING = 2, 3, 4
NT = F // TF
NU = TWO * MATS * NT
NA = TWO * NT + TWO
DEEP = 6
LANES, SUB, HALF, CH, SH = 128, 80, 512, 256, 400
NCH = 2
DEV = D // LANES
TF2, TF3, TB = TWO * TF, MATS * TF, T // TWO
TC = TB // NCH
AROWS = LANES // DEV
OFFS = range(1, RING)
VMEM_LIMIT = 67043328
EPS = 1e-6
OFFLAY = NU // TWO


def sds(s, d): return jax.ShapeDtypeStruct(s, d)
def dot_(a, b, ca, cb): return lax.dot_general(a, b, (((ca,), (cb,)), ((), ())), preferred_element_type=f32)
def mul(i, n): return pl.multiple_of(i * n, n)
def blk(i, n): return pl.ds(mul(i, n), n)
def cut(n): return pl.ds(0, n)
def cpy(src, dst, sem): return pltpu.make_async_copy(src, dst, sem)
def wt(ref, sem): cpy(ref, ref, sem).wait()
def start(cs):
    for q in cs: q.start()
def each(lo, hi, f):
    def g(i, _):
        f(i)
        return _
    lax.fori_loop(lo, hi, g, 0)
def rms(wide): return lax.rsqrt(jnp.mean(wide * wide, -1, keepdims=True) + EPS)
def pc(k): return (k % TWO) * RING + k // TWO
def par(u): return u % TWO
def ring(u): return u % RING


def step_kernel(x_h, dy_h, wg_i, wu_i, wd_i,
                gt_o, gd_o, sq_o, WGU, WD, a0p_h, h1p_h, AB_h, h_h,
                ya, acc, wgu, wdb, H, G, R0, Pb, R1, Q, R2, U, R3, GT, sqa, SQ,
                dysem, asem, psem, ownsem, gusem, wdsem, stsem, hsem, gtsem, locsem,
                s0s, s0r, s1s, s1r, s2s, s2r, s3s, s3r, s4s, s4r, a2s, a2r,
                ag0s, ag0r, agds, agdr, ag1s, ag1r, ag2s, ag2r, sqs, sqr):
    r_, me = lax.axis_index("r"), lax.axis_index("s")
    x, y, z, c = me // TWO, r_ // RING, r_ % RING, me % TWO
    own = c * RING + x
    def dev(x, y, z, c): return (0, y * RING + z, x * TWO + c)
    def xdev(d): return dev(ring(x + d), y, z, c)
    def ydev(d): return dev(x, ring(y + d), z, c)
    def zdev(d): return dev(x, y, ring(z + d), c)
    part = dev(x, y, z, 1 - c)
    AX = ((0, y, ydev), (1, z, zdev))
    dyp, ap = ya.at[0], ya.at[1]
    bar = pltpu.get_barrier_semaphore()
    peers = [part] + [f(d) for f in (xdev, ydev, zdev) for d in OFFS] + [dev(ring(x + d), y, z, 1 - c) for d in OFFS]
    for p in peers: pl.semaphore_signal(bar, inc=1, device_id=p, device_id_type=pl.DeviceIdType.MESH)
    def rd(src, dst, ss, rs, d):
        return pltpu.make_async_remote_copy(src_ref=src, dst_ref=dst, send_sem=ss, recv_sem=rs, device_id=d, device_id_type=pl.DeviceIdType.MESH)
    def same(ref, ss, rs, d): return rd(ref, ref, ss, rs, d)
    def permuted(src, dst, sem): return [cpy(src.at[:, pl.ds(k * LANES, LANES)], dst.at[:, pl.ds(pc(k) * LANES, LANES)], sem) for k in range(DEV)]
    start(permuted(x_h, ap, psem))
    staged = [wdb.at[pl.ds(l * TF, SH)] for l in range(TWO)]
    for l in range(TWO): start(permuted(wd_i.at[l], staged[l], ownsem.at[l]))
    start(permuted(dy_h, dyp, dysem))
    sqa[...] = jnp.zeros_like(sqa)
    pl.semaphore_wait(bar, len(peers))

    def gu_load(l, j, b):
        for m, inp in enumerate((wg_i, wu_i)):
            cols = pl.ds(m * TF, TF)
            cpy(inp.at[l, :, blk(j, TF)], wgu.at[b, blk(own, LANES), cols], gusem.at[b]).start()
            def one(e):
                k = (own + e) % DEV
                cpy(WGU.at[l, k, m, :, blk(j, TF)], wgu.at[b, blk(k, LANES), cols], gusem.at[b]).start()
            each(1, DEV, one)
    def gu_wait(b): wt(wgu.at[b], gusem.at[b])
    def d_load(l, j, b): cpy(WD.at[l, blk(j, TF), :], wdb.at[blk(b, TF)], wdsem.at[b]).start()
    def d_wait(b): wt(wdb.at[blk(b, TF)], wdsem.at[b])

    def q16(h, q): return pl.ds(pl.multiple_of(h * (LANES // TWO) + q * AROWS, AROWS), AROWS)
    def colq(h, q): return blk(pc(RING * h + q), LANES)
    def fork(u, fg, fd):
        @pl.when(u % (NT + TWO) < NT)
        def _(): fg(u // (NT + TWO), u % (NT + TWO))
        @pl.when(u % (NT + TWO) >= NT)
        def _(): fd(u - NT)
    def both(ref, ss, rs, b):
        wt(ref, ss.at[b])
        wt(ref, rs.at[b])
    def A0(u):
        b = u % DEEP
        def fg(l, j):
            for m, inp in enumerate((wg_i, wu_i)):
                def one(i):
                    for h, q, _ in AX: rd(inp.at[l, q16(h, q), blk(j, TF)], WGU.at[l, own, m, q16(h, q), blk(j, TF)], ag0s.at[b], ag0r.at[b], xdev(i + 1)).start()
                each(0, MATS, one)
                rd(inp.at[l, :, blk(j, TF)], WGU.at[l, own, m, :, blk(j, TF)], agds.at[u], agdr.at[u], part).start()
        def fd(l):
            wt(WD.at[0, cut(SH), :], ownsem.at[l])
            def one(i):
                for h, q, _ in AX: same(WD.at[l, blk(me, SH), colq(h, q)], ag0s.at[b], ag0r.at[b], xdev(i + 1)).start()
            each(0, MATS, one)
            same(WD.at[l, blk(me, SH), :], agds.at[u], agdr.at[u], part).start()
        fork(u, fg, fd)
    def A1(u):
        b = u % DEEP
        def fg(l, j):
            both(WGU.at[0, cut(DEEP), :, cut(AROWS), cut(TF)], ag0s, ag0r, b)
            def one(i):
                k, d = c * RING + ring(x + i // MATS + 1), i % MATS
                for h, q, f in AX: same(WGU.at[l, k, :, q16(h, q), blk(j, TF)], ag1s.at[b], ag1r.at[b], f(d + 1)).start()
            each(0, MATS * MATS, one)
        def fd(l):
            both(WD.at[0, cut(DEEP * SH), cut(LANES)], ag0s, ag0r, b)
            def one(i):
                k, d = TWO * ring(x + i // MATS + 1) + c, i % MATS
                for h, q, f in AX: same(WD.at[l, blk(k, SH), colq(h, q)], ag1s.at[b], ag1r.at[b], f(d + 1)).start()
            each(0, MATS * MATS, one)
        fork(u, fg, fd)
    gu1, gu3 = WGU.at[0, 0, :, :, cut(TF)], WGU.at[0, cut(MATS), :, :, cut(TF)]
    wd1, wd3 = WD.at[0, cut(SH), :], WD.at[0, cut(MATS * SH), :]
    def A2(u):
        b = u % DEEP
        def fg(l, j):
            both(WGU.at[0, cut(DEEP), :, cut(MATS * AROWS), cut(TF)], ag1s, ag1r, b)
            each(1, RING, lambda i: same(WGU.at[l, c * RING + ring(x + i), :, :, blk(j, TF)], ag2s.at[b], ag2r.at[u], part).start())
        def fd(l):
            both(WD.at[0, cut(DEEP * SH), cut(MATS * LANES)], ag1s, ag1r, b)
            each(1, RING, lambda i: same(WD.at[l, blk(TWO * ring(x + i) + c, SH), :], ag2s.at[b], ag2r.at[u], part).start())
        fork(u, fg, fd)
    def A3(u):
        b = u % DEEP
        def done(one, three):
            for ref, sem in ((one, agds.at[u]), (one, agdr.at[u]), (three, ag2s.at[b]), (three, ag2r.at[u])): wt(ref, sem)
        fork(u, lambda l, j: done(gu1, gu3), lambda l: done(wd1, wd3))
    def guard(A, u):
        @pl.when(jnp.logical_and(u >= 0, u < NA))
        def _(): A(u)

    def c0(u): return rd(G.at[par(u), :, blk(1 - c, HALF)], R0.at[ring(u)], s0s.at[par(u)], s0r.at[ring(u)], part)
    def mat_(u): return u % MATS
    def deep(u): return u % DEEP
    def c1(u):
        return [rd(Pb.at[mat_(u), h, ring(q + d)], R1.at[ring(u), h, d - 1], s1s.at[ring(u)], s1r.at[ring(u)], f(d)) for d in OFFS for h, q, f in AX]
    def c1x(u): return [rd(Pb.at[mat_(u), :, :, ring(x + d)], R1.at[ring(u), :, d - 1], s1s.at[ring(u)], s1r.at[ring(u)], xdev(d)) for d in OFFS]
    def c2(u): return [rd(Q.at[ring(u), ring(x + d)], R2.at[deep(u), d - 1], s2s.at[ring(u)], s2r.at[deep(u)], xdev(d)) for d in OFFS]
    def c2x(u):
        return [rd(Q.at[ring(u), ring(q + d), h], R2.at[deep(u), d - 1, h], s2s.at[ring(u)], s2r.at[deep(u)], f(d)) for d in OFFS for h, q, f in AX]
    def either(u, f, *args):
        @pl.when(mat_(u) > 0)
        def _(): f(*args[0])
        @pl.when(mat_(u) == 0)
        def _(): f(*args[1])
    def c3(u):
        return [rd(U.at[ring(u), h], R3.at[deep(u), h, q], s3s.at[ring(u)], s3r.at[deep(u)], f(d)) for d in OFFS for h, q, f in ((0, z, zdev), (1, y, ydev))]
    def rows(h, q): return pl.ds(pl.multiple_of(h * (TF // TWO) + q * SUB, SUB), SUB)
    def c4(u):
        return [same(GT.at[u, rows(h, q)], s4s.at[ring(u)], s4r.at[deep(u)], f(d)) for d in OFFS for h, q, f in AX]
    def S0(u): c0(u).start()
    def S1(u):
        c0(u).wait()
        for i in range(DEV):
            for k in range(RING):
                mine = G[par(u), pl.ds(i * SUB, SUB), blk(c * RING + k, LANES)]
                Pb[mat_(u), i // RING, i % RING, k] = (mine.astype(f32) + R0[ring(u), pl.ds(i * SUB, SUB), pl.ds(k * LANES, LANES)].astype(f32)).astype(bf)
        either(u, lambda way: start(way(u)), (c1,), (c1x,))
    def added(first, rest):
        s = first.astype(f32)
        for q in rest: s = s + q.astype(f32)
        return s.astype(bf)
    def second(u, first, send):
        wt(R1.at[0], s1s.at[ring(u)])
        wt(R1.at[0], s1r.at[ring(u)])
        for h, mine, _ in AX:
            for k in range(RING): Q[ring(u), k, h] = added(first(h, mine, k), [R1[ring(u), h, d, k] for d in range(MATS)])
        start(send(u))
    def S2(u):
        @pl.when(mat_(u) > 0)
        def _(): second(u, lambda h, mine, k: Pb[mat_(u), h, mine, k], c2)
    def S2x(u):
        @pl.when(mat_(u) == 0)
        def _(): second(u, lambda h, mine, k: Pb[mat_(u), h, k, x], c2x)
    def S3(u):
        wt(R2.at[0], s2s.at[ring(u)])
        wt(R2.at[0], s2r.at[deep(u)])
        def go(*mine):
            for h in range(TWO): U[ring(u), h] = added(Q[ring(u), mine[h], h], [R2[deep(u), d, h] for d in range(MATS)])
        either(u, go, (x, x), (y, z))
        start(c3(u))
    def S4(u):
        wt(R2.at[0], s3s.at[ring(u)])
        wt(R2.at[0], s3r.at[deep(u)])
        R3[deep(u), 0, z] = U[ring(u), 0]
        R3[deep(u), 1, y] = U[ring(u), 1]
        for h, q, _ in AX:
            s = R3[deep(u), h, 0].astype(f32)
            for d in OFFS: s = s + R3[deep(u), h, d].astype(f32)
            GT[u, rows(h, q)] = s.astype(bf)
        start(c4(u))
    def a2a(u, i):
        lay, n = u // OFFLAY, DEV * ((u % OFFLAY) // MATS) + i
        to = n // NT
        src, dst = GT.at[u, blk(i, SUB)], gd_o.at[1 - lay, blk(n - NT * to, SUB), blk(me, LANES)]
        @pl.when(to != me)
        def _(): rd(src, dst, a2s, a2r.at[lay], (0, r_, to)).start()
        @pl.when(to == me)
        def _(): cpy(src, dst, locsem).start()
    def S5(u):
        wt(R2.at[0], s4s.at[ring(u)])
        wt(R2.at[0], s4r.at[deep(u)])
        v = GT[u].astype(f32)
        sqa[...] += jnp.sum((v * v).reshape(SUB, DEV, LANES), axis=0)
        @pl.when(u % MATS > 0)
        def _(): cpy(GT.at[u], gt_o.at[u], gtsem).start()
        @pl.when(u % MATS == 0)
        def _():
            each(0, DEV, lambda i: a2a(u, i))
    LAST = TWO * len((S1, S2, S3, S4, S5))
    STAGES = ((S2, RING, NU), (S2x, NT, NU), (S3, LAST - RING, NU), (S1, TWO, NU - 1), (S4, LAST - TWO, NU), (S5, LAST, NU))
    def slot(t):
        for S, lag, end in STAGES:
            @pl.when(jnp.logical_and(t >= lag, t < end + lag))
            def _(): S(t - lag)
            if S is S1:
                @pl.when(t == NU)
                def _(): S1(t - 1)

    each(0, MATS, A0)
    for l in range(TWO):
        wt(staged[l], ownsem.at[l])
        cpy(staged[l], WD.at[l, blk(me, SH), :], ownsem.at[l]).start()
    wt(ap, psem)
    def xnorm(i):
        wide = ya[1, blk(i, CH), :].astype(f32)
        ya[1, blk(i, CH), :] = (wide * rms(wide)).astype(bf)
    each(0, T // CH, xnorm)
    cpy(ap, a0p_h, asem).start()
    def head(i):
        guard(A2, i - 1)
        @pl.when(i == 0)
        def _(): A1(i)
        A1(i + 1)
        A0(i + MATS)
    each(0, TWO, head)
    each(0, 1, A3)
    gu_load(0, 0, 0)
    each(MATS, RING, A1)
    each(NT, DEEP, A0)
    def stv(i): return acc.at[blk(i, TF2), :]
    def step1(j):
        b = par(j)
        gu_wait(b)
        hs = j % MATS
        hr = blk(hs, TF)
        @pl.when(j >= MATS)
        def _(): wt(H.at[cut(TF)], hsem.at[hs])
        guard(A2, j + 1)
        def sub(s):
            @pl.when(j > 0)
            def _(): wt(stv(0), stsem.at[s])
            for q in range(NCH):
                t, cols = pl.ds(pl.multiple_of(s * TB + q * TC, TC), TC), pl.ds(q * TC, TC)
                gu = dot_(wgu[b], ya[1, t, :], 0, 1)
                g, u = gu[:TF], gu[TF:]
                sg = jax.nn.sigmoid(g)
                si = g * sg
                acc[pl.ds(mul(s, TF2), TF), cols] = si
                acc[pl.ds(pl.multiple_of(s * TF2 + TF, TF), TF), cols] = u * (sg + si * (1 - sg))
                H[hr, t] = (si * u).astype(bf)
            cpy(stv(s), AB_h.at[TWO * j + s], stsem.at[s]).start()
            @pl.when(s == 0)
            def _():
                guard(A3, j + 1)
                @pl.when(j < NT - 1)
                def _(): gu_load(0, j + 1, 1 - b)
                @pl.when(j == NT - 1)
                def _(): cpy(WD.at[0, pl.ds(TF3, TF2), :], wdb, wdsem.at[TWO]).start()
                guard(A1, j + RING)
                guard(A0, j + DEEP)
        each(0, TWO, sub)
        cpy(H.at[hr], h_h.at[blk(j, TF), :], hsem.at[hs]).start()
    each(0, NT, step1)
    for i in range(TWO): wt(stv(0), stsem.at[i])
    wt(ap, asem)
    start(permuted(x_h, ap, psem))
    lo, mid = cut(TF2), wgu.at[0, cut(TF), cut(D)]
    cpy(WD.at[0, pl.ds(TF2, TF), :], mid, wdsem.at[0]).start()
    def down(i):
        @pl.when(i == 1)
        def _(): wt(H.at[lo], hsem.at[MATS])
        wt(wdb, wdsem.at[TWO])
        def halves(h):
            term = lambda: dot_(H[lo, blk(h, TB)], wdb[...], 0, 0)
            @pl.when(i == 0)
            def _(): acc[blk(h, TB), :] = term()
            @pl.when(i > 0)
            def _(): acc[blk(h, TB), :] += term()
        each(0, TWO, halves)
        @pl.when(i == 0)
        def _():
            for k in range(TWO): wt(H.at[cut(TF)], hsem.at[k])
            cpy(h_h.at[lo], H.at[lo], hsem.at[MATS]).start()
            cpy(WD.at[0, lo, :], wdb, wdsem.at[TWO]).start()
            A2(i + DEEP)
            A1(i + NA - MATS)
            A0(i + NA - 1)
            wt(mid, wdsem.at[0])
            def halves(h): acc[blk(h, TB), :] += dot_(H[TF2:TF3, blk(h, TB)], wgu[0, 0:TF, 0:D], 0, 0)
            each(0, TWO, halves)
        A3(i + DEEP)
        A2(i + DEEP + 1)
        @pl.when(i == 0)
        def _(): A1(i + NA - TWO)
    each(0, TWO, down)
    gu_load(1, 0, 1)
    d_load(1, 0, 0)
    wt(H.at[cut(TF)], hsem.at[TWO])
    wt(ap, psem)
    def h1s(b): return G.at[b, cut(CH)]
    def fin(i):
        b, r = par(i), blk(i, CH)
        @pl.when(i >= TWO)
        def _(): wt(h1s(0), hsem.at[b])
        h1 = (ya[1, r, :].astype(f32) + acc[r, :].astype(bf).astype(f32)).astype(bf)
        G[b, 0:CH] = h1
        cpy(h1s(b), h1p_h.at[r], hsem.at[b]).start()
        wide = h1.astype(f32)
        ya[1, r, :] = (wide * rms(wide)).astype(bf)
        acc[r, :] = jnp.zeros((CH, D), f32)
    each(0, T // CH, fin)
    for b in range(TWO): wt(h1s(0), hsem.at[b])
    def after(i):
        A3(i)
        A1(i + MATS)
    each(DEEP + TWO, DEEP + MATS, after)
    wt(dyp, dysem)

    def h1l(k): return cpy(h1p_h.at[pl.ds(k * D, D)], H.at[cut(D), pl.ds(k * D, D)], hsem.at[k])
    def abl(j, s): return cpy(AB_h.at[TWO * j + s], stv(s), stsem.at[s])
    def hload(j): return cpy(h_h.at[blk(j, TF), :], H.at[cut(TF)], hsem.at[TWO])
    def layer1(k, b):
        gu_wait(b)
        @pl.when(k + 1 < NT)
        def _(): gu_load(1, k + 1, 1 - b)
        def half(h):
            for q in range(NCH):
                t = pl.ds(pl.multiple_of(h * TB + q * TC, TC), TC)
                gu = dot_(wgu[b], ya[1, t, :], 0, 1)
                g, u = gu[:TF], gu[TF:]
                dh = dot_(wdb[blk(par(k), TF)], ya[0, t, :], 1, 1).astype(bf).astype(f32)
                sg = jax.nn.sigmoid(g)
                si = g * sg
                H[0:TF, t] = (si * u).astype(bf)
                H[TF2:TF3, t] = (dh * si).astype(bf)
                H[TF:TF2, t] = (dh * u * (sg + si * (1 - sg))).astype(bf)
            @pl.when(h == 0)
            def _(): guard(A2, k + DEEP + MATS)
        each(0, TWO, half)
        guard(A3, k + DEEP + MATS)
    def between():
        cpy(a0p_h, ap, asem).start()
        for k in range(TWO): wt(H.at[cut(D), cut(D)], hsem.at[k])
        def nb(i):
            r = blk(i, CH)
            wide = H[blk(ring(i), CH), blk(i // RING, D)].astype(f32)
            scale = rms(wide)
            da = acc[r, :].astype(bf).astype(f32)
            inner = jnp.mean(da * wide, -1, keepdims=True)
            dw = (da * scale - wide * (scale * scale * scale * inner)).astype(bf)
            ya[0, r, :] = (ya[0, r, :].astype(f32) + dw.astype(f32)).astype(bf)
            @pl.when(i == TF2 // CH - 1)
            def _(): abl(0, 0).start()
        each(0, T // CH, nb)
        abl(0, 1).start()
        hload(0).start()
        wt(ap, asem)
    def layer0(j, b):
        def sub(s):
            abl(j, s).wait()
            for q in range(NCH):
                t, cols = pl.ds(pl.multiple_of(s * TB + q * TC, TC), TC), pl.ds(q * TC, TC)
                dh = dot_(wdb[blk(b, TF)], ya[0, t, :], 1, 1).astype(bf).astype(f32)
                H[TF2:TF3, t] = (dh * acc[pl.ds(mul(s, TF2), TF), cols]).astype(bf)
                H[TF:TF2, t] = (dh * acc[pl.ds(pl.multiple_of(s * TF2 + TF, TF), TF), cols]).astype(bf)
            @pl.when(j + 1 < NT)
            def _(): abl(j + 1, s).start()
        each(0, TWO, sub)
        hload(j).wait()
    def tile(k):
        b, gb = par(k), par(k + 1)
        d_wait(b)
        @pl.when(k + 1 < NT)
        def _(): d_load(1, k + 1, 1 - b)
        @pl.when(jnp.logical_and(k + 1 >= NT, k + 1 < TWO * NT))
        def _(): d_load(0, k + 1 - NT, 1 - b)
        @pl.when(k < NT)
        def _(): layer1(k, gb)
        @pl.when(k == NT)
        def _(): between()
        @pl.when(k >= NT)
        def _(): layer0(k - NT, b)
        def mat(m):
            t = MATS * k + m
            slot(t)
            G[par(t)] = dot_(H[blk(m, TF)], ya[(m + 1) // TWO], 1, 0).astype(bf)
            S0(t)
            @pl.when(jnp.logical_and(k < NT, m < TWO))
            def _(): acc[blk(m, TB), :] += dot_(H[TF:TF3, blk(m, TB)], wgu[gb], 0, 1)
            @pl.when(jnp.logical_and(k == NT - 1, m == 1))
            def _():
                for q in range(TWO): h1l(q).start()
            @pl.when(jnp.logical_and(jnp.logical_and(k >= NT, k + 1 < TWO * NT), m == 0))
            def _(): hload(k - NT + 1).start()
        each(0, MATS, mat)
    each(0, TWO * NT, tile)
    each(NU, NU + LAST, slot)

    SQ[me] = sqa[...]
    def sqc(e, i): return rd(sqa, SQ.at[i], sqs, sqr, (0, r_, (me + e) % DEV))
    for e in range(1, DEV): sqc(e, me).start()
    def drain(n, k, sem): wt(GT.at[cut(n), cut(k)], sem)
    drain(NU - TWO * NT, TF, gtsem)
    drain(TWO, SH, locsem)
    drain(TWO * (DEV - 1), SH, a2s)
    for l in range(TWO): drain(DEV - 1, SH, a2r.at[l])
    for sem in (sqs, sqr): wt(SQ.at[cut(DEV - 1)], sem)
    tot = SQ[0]
    for i in range(1, DEV): tot = tot + SQ[i]
    sq_o[...] = tot


def train(x, dy, wg, wu, wd):
    hbm = pl.BlockSpec(memory_space=pl.ANY)
    V, S = pltpu.VMEM, pltpu.SemaphoreType.DMA
    b = (SUB, LANES)
    r3 = (RING, TWO, MATS)
    one, two, three, four, six = S, S((TWO,)), S((MATS,)), S((RING,)), S((DEEP,))
    outs = [sds((NU, TF, LANES), bf), sds((TWO, SH, D), bf), sds((DEV, LANES), f32), sds((TWO, DEV, TWO, LANES, F), bf), sds((TWO, F, D), bf),
            sds((T, D), bf), sds((T, D), bf), sds((NT * TWO, TF2, D), f32), sds((F, T), bf)]
    specs = [hbm] * len(outs)
    specs[TWO] = pl.BlockSpec(memory_space=pltpu.VMEM)
    return pl.pallas_call(
        step_kernel,
        out_shape=outs, in_specs=[hbm] * (MATS + TWO), out_specs=specs,
        scratch_shapes=[
            V((TWO, T, D), bf), V((TWO * TF2, D), f32), V((TWO, D, TF2), bf), V((TF2, D), bf), V((TF3, T), bf), V((TWO, TF, D), bf), V((RING, TF, HALF), bf),
            V((MATS, TWO, RING, RING) + b, bf), V(r3 + (RING,) + b, bf), V((RING, RING, TWO) + b, bf), V((DEEP, MATS, TWO) + b, bf), V((RING, TWO) + b, bf), V((DEEP, TWO, RING) + b, bf),
            V((NU, TF, LANES), bf), V((DEV, LANES), f32), V((DEV, DEV, LANES), f32),
            one, one, one, two, two, three, two, S((RING,)), one, one,
            two, four, four, four, four, six, four, six, four, six, one, two,
            six, six, S((NA,)), S((NA,)), six, six, six, S((NA,)), one, one],
        compiler_params=pltpu.CompilerParams(collective_id=0, has_side_effects=True, vmem_limit_bytes=VMEM_LIMIT),
        name="train")(x, dy, wg, wu, wd)


def optimizer(sq, GT, GD, w, m, v):
    groups = [(l, i) for l in range(TWO) for i in range(MATS)]
    def kernel(sq, GT, GD, *r):
        take = lambda k: r[k * MATS:(k + 1) * MATS]
        srcs, dsts, bufs = [take(k) for k in range(MATS)], [take(k) for k in range(MATS, DEEP)], [take(k) for k in range(DEEP, DEEP + MATS)]
        gb, gdb, isem, osem, gsem = r[MATS * (DEEP + MATS):]
        for l, i in groups:
            for k in range(MATS): cpy(srcs[k][i].at[l], bufs[k][i].at[l], isem.at[k, l, i]).start()
            if i == TWO: cpy(GD.at[l], gdb.at[l], gsem.at[l, i]).start()
            else: start([cpy(GT.at[(1 - l) * OFFLAY + MATS * j + i + 1], gb.at[l, i, j], gsem.at[l, i]) for j in range(NT)])
        tot = jnp.sum(jnp.sum(sq[...], axis=0, keepdims=True), axis=1, keepdims=True)
        factor = jnp.minimum(1.0, 0.5 * lax.rsqrt(tot / (TWO * MATS * D * F) + 1e-30))
        for l, i in groups:
            for k in range(MATS): wt(bufs[k][i].at[l], isem.at[k, l, i])
            wt(gdb.at[l] if i == TWO else gb.at[l, i], gsem.at[l, i])
            wb, mb, vb = (bufs[k][i] for k in range(MATS))
            def one(j):
                at = (l, blk(j, SUB), slice(None)) if i == TWO else (l, slice(None), blk(j, TF))
                g = (gdb[at].astype(f32) if i == TWO else gb[l, i, j].astype(f32).T) * factor
                mm = 0.9 * mb[at] + 0.1 * g
                vv = 0.95 * vb[at] + 0.05 * g * g
                ww = wb[at].astype(f32)
                wb[at] = (ww - 0.02 * (mm * lax.rsqrt(vv + 1e-8) + 0.1 * ww)).astype(bf)
                mb[at], vb[at] = mm, vv
                for k in range(MATS): cpy(bufs[k][i].at[at], dsts[k][i].at[at], osem.at[k, l, i]).start()
            each(0, NT, one)
        for l, i in groups:
            for k in range(MATS): wt(bufs[k][i].at[l], osem.at[k, l, i])
    hbm = pl.BlockSpec(memory_space=pl.ANY)
    V, S = pltpu.VMEM, pltpu.SemaphoreType.DMA
    outs = tuple(sds(q.shape, t) for t in (bf, f32, f32) for q in w)
    return pl.pallas_call(
        kernel, in_specs=[pl.BlockSpec(memory_space=pltpu.VMEM)] + [hbm] * (TWO + MATS * MATS), out_specs=(hbm,) * len(outs), out_shape=outs,
        scratch_shapes=[V(q.shape, q.dtype) for q in outs] + [V((TWO, TWO, NT, TF, LANES), bf), V((TWO, SH, D), bf), S((MATS, TWO, MATS)), S((MATS, TWO, MATS)), S((TWO, MATS))],
        compiler_params=pltpu.CompilerParams(vmem_limit_bytes=VMEM_LIMIT),
        name="optimizer")(sq, GT, GD, *w, *m, *v)


def solution(mesh):
    def step(x, dy, *arrays):
        w, m, v = (arrays[i:i + MATS] for i in range(0, len(arrays), MATS))
        GT, GD, sq = train(x[0], dy[0], *w)[:MATS]
        return optimizer(sq, GT, GD, w, m, v)
    states, cuts = P(("rep", "r", "s"), None, None), P(None, "s", None)
    return jax.shard_map(step, mesh=mesh, in_specs=(states, states) + (cuts,) * (MATS * MATS), out_specs=(P("rep", "s", None),) * (MATS * MATS), check_vma=False)
```
